32 devices in a mesh: dp: 4 (over y, x), expert: 8 (over z, core).
Axes of the slice: x: 2, y: 2, z: 4, core: 2. Of those that a mesh axis runs over, the one named last changes fastest.
Arguments:
- residual_in: bfloat16 [4096, 2048], P(('dp', 'expert')), may hold values from -6 to 6
- queries: bfloat16 [4096, 2048], P(('dp', 'expert')), may hold values from -6 to 6
- keys_in: bfloat16 [4096, 2048], P(('dp', 'expert')), may hold values from -6 to 6
- values_in: bfloat16 [4096, 2048], P(('dp', 'expert')), may hold values from -6 to 6
- out_gate: bfloat16 [4096, 2048], P(('dp', 'expert')), may hold values from -6 to 6
- log_decay: float32 [16, 4096], P(None, ('dp', 'expert')), may hold values from -0.7 to 0
- beta_rate: float32 [16, 4096], P(None, ('dp', 'expert')), may hold values from 0.05 to 0.95
- head_gain: float32 [128], replicated, may hold values from 0.1 to 1.9
- moe_gain: float32 [2048], replicated, may hold values from 0.1 to 1.9
- state_cache: float32 [32, 2, 16, 128, 128], P(('dp', 'expert')), may hold values from -1.8 to 1.8
- hit_holder: int32 [32], P(('dp', 'expert')), may hold values from 0 to 3
- hit_slot: int32 [32], P(('dp', 'expert')), may hold values from 0 to 1
- expert_ids: int32 [4096, 10], P(('dp', 'expert')), may hold values from 0 to 31, all different within a row; in each aligned block of 128 rows (0 to 127, 128 to 255, ...) at most 56 rows name the same one
- gate_weight: float32 [4096, 10], P(('dp', 'expert')), may hold values from 0.03 to 0.3
- w_gate: bfloat16 [32, 2048, 512], P('expert'), may hold values from -0.125 to 0.125
- w_up: bfloat16 [32, 2048, 512], P('expert'), may hold values from -0.125 to 0.125
- w_down: bfloat16 [32, 512, 2048], P('expert'), may hold values from -0.25 to 0.25
Outputs:
- mixer_out: bfloat16 [4096, 2048], P(('dp', 'expert'))
- expert_out: bfloat16 [4096, 2048], P(('dp', 'expert'))
- next_state: float32 [32, 16, 128, 128], P(('dp', 'expert'))
The draws below stay inside these ranges and needn't reach their ends.
Inputs may be any that keep to these rules, and one draw needn't show every extreme that they name: `expert_ids`: within the 128 rows of one device no expert is named by more than 56 of them, and the 10 numbers of a row differ.
All inputs are finite; a program needn't handle non-finite values.
Results may differ from the reference program's by a relative error of at most 0.014.
Values may be sent and summed in bfloat16 or wider, within the bound.
No kernel may reach another device: no remote copies, remote signals or barrier semaphores. Data moves between devices by JAX's collectives and lax.ppermute only.
A program may use at most 128 MiB of HBM per device.

```python
import math
import jax
import jax.numpy as jnp
import numpy as np
from jax import lax

D = 2048
OUTPUT_CHANNELS = 16
DK = 128
DV = 128
FF = 512
TOPK = 10
EXPERTS = 32
SHARD_LENGTH = 128
SLOTS = 2
MOST = 56
GROUP = 8
HOLDERS = 4
SHARD_TOTAL = 32
TOKENS = 4096


def draw_log_decay(key, part):
    lookup_vectors = jax.random.split(key, 7)
    slow_share = 0.5
    slow = jax.random.uniform(lookup_vectors[0], (OUTPUT_CHANNELS, 1, 1)) < slow_share
    slow_total = jnp.exp(jax.random.uniform(lookup_vectors[1], (OUTPUT_CHANNELS, 1, 1), minval=jnp.log(0.03), maxval=jnp.log(0.5)))
    slow_step = slow_total / SHARD_LENGTH
    fast_step = 1.0 / jax.random.uniform(lookup_vectors[2], (OUTPUT_CHANNELS, 1, 1), minval=20.0, maxval=50.0)
    floor_amount = jnp.where(slow, slow_step, fast_step)
    shard_scaling_factor = jnp.exp(jax.random.uniform(lookup_vectors[3], (OUTPUT_CHANNELS, SHARD_TOTAL, 1), minval=jnp.log(0.5), maxval=jnp.log(2.0)))
    rough_estimate = jax.random.uniform(lookup_vectors[4], (OUTPUT_CHANNELS, SHARD_TOTAL, SHARD_LENGTH), minval=0.5, maxval=1.5)
    spike_location = jax.random.uniform(lookup_vectors[5], (1, SHARD_TOTAL, SHARD_LENGTH)) < 2.0 / SHARD_LENGTH
    spike_surcharge = jax.random.uniform(lookup_vectors[6], (OUTPUT_CHANNELS, SHARD_TOTAL, SHARD_LENGTH), minval=0.2, maxval=0.4)
    payload_vectors = -floor_amount * shard_scaling_factor * rough_estimate + jnp.where(spike_location, jnp.log1p(-spike_surcharge), 0.0)
    return payload_vectors.reshape(OUTPUT_CHANNELS, SHARD_TOTAL * SHARD_LENGTH).astype(jnp.float32)


def touch_ends(drawn, key, smallest, largest):
    shape = drawn.shape
    index_at = [jax.random.randint(jax.random.fold_in(key, axis), (), 0, shape[axis]) for axis in range(len(shape))]
    drawn = drawn.at[tuple(index_at)].set(smallest)
    longest = shape.index(max(shape))
    index_at[longest] = (index_at[longest] + 1) % shape[longest]
    return drawn.at[tuple(index_at)].set(largest)


def block_scale(stream_key, dims, shards, low, top_value):
    def one(axis_at, blocks):
        draws = jax.random.uniform(jax.random.fold_in(jax.random.fold_in(stream_key, 6), axis_at), (blocks,), jnp.float32, low / len(shards), top_value / len(shards))
        return jnp.repeat(jnp.exp(draws), dims[axis_at] // blocks).reshape((-1,) + (1,) * (len(dims) - axis_at - 1))

    level = one(*shards[0])
    for cut in shards[1:]:
        level = level * one(*cut)
    return level


def rank_table(count, slope):
    loads = [(1 << 20) // math.isqrt(rank ** slope) + 1 for rank in range(1, count + 1)]
    spread = 1 + sum(loads) // (1 << 30)
    return np.cumsum(np.array([max(1, weight // spread) for weight in loads]))


def ranked(rng, shape, count, skew):
    table = rank_table(count, skew)
    lot = jax.random.randint(jax.random.fold_in(rng, 1), shape, 0, int(table[count - 1]))
    grade = jnp.searchsorted(jnp.asarray(table, jnp.int32), lot, side="right")
    return jax.random.permutation(jax.random.fold_in(rng, 2), count)[grade].astype(jnp.int32)


def deal_out(key, own, number, rows, amount, top, bound, skew):
    sequence = jax.random.permutation(key, amount)
    crowded, usual = shares(amount, rows * top, bound, skew, True), shares(amount, rows * top, bound, skew, False)
    places = jnp.arange(amount)

    def named(sizes, turn):
        used = int((sizes > 0).sum())
        fixed = max(1, used // 4)
        passed = fixed + (places - fixed + turn * (used - fixed)) % max(1, amount - fixed)
        return jnp.zeros((amount,), jnp.int32).at[sequence[jnp.where(places < fixed, places, passed)]].set(jnp.asarray(sizes, jnp.int32))

    sizes = jnp.where(number % 4 == 0, named(crowded, number // 4), named(usual, number - number // 4 - 1))
    mixed = jax.random.permutation(jax.random.fold_in(own, 3), amount)
    source_of, receiver = mixed[0:amount // 2 * 2:2], mixed[1:amount // 2 * 2:2]
    slack = jnp.minimum(sizes[source_of] - 1, bound - sizes[receiver]) // 2
    slack = jnp.where((source_of == sequence[0]) | (receiver == sequence[0]) | (sizes[receiver] == 0), 0, jnp.maximum(slack, 0))
    passed = jax.random.randint(jax.random.fold_in(own, 4), (amount // 2,), 0, 1 << 20) % (slack + 1)
    sizes = sizes.at[source_of].add(-passed).at[receiver].add(passed)
    items = jnp.searchsorted(jnp.cumsum(sizes), jnp.arange(rows * top), side="right").astype(jnp.int32)
    table = items.reshape(top, rows).T
    table = table[jax.random.permutation(jax.random.fold_in(own, 1), rows)]
    turn = jax.random.randint(jax.random.fold_in(own, 2), (rows, 1), 0, top)
    return jnp.take_along_axis(table, (jnp.arange(top)[None, :] + turn) % top, axis=1)


def shares(amount, total, reach, slope, full):
    loads = [(1 << 20) // math.isqrt(rank ** slope) + 1 for rank in range(1, amount + 1)]
    largest = reach if full else min(reach, max(-(-total // amount), total * loads[0] // sum(loads)))
    least = 1 if total - largest >= amount - 1 else 0
    counts, surplus = [largest] + [least] * (amount - 1), total - largest - least * (amount - 1)
    while surplus > 0:
        movable = [i for i in range(1, amount) if counts[i] < largest] or [i for i in range(1, amount) if counts[i] < reach]
        mass, left = sum([loads[i] for i in movable]), surplus
        for i in movable:
            extra = min(reach - counts[i], max(1, left * loads[i] // mass), surplus)
            counts[i] = counts[i] + extra
            surplus = surplus - extra
    return np.array(counts)


def scatter_about(stream_key, shape, spread, most, cuts=(), held_as=jnp.bfloat16):
    drawn = spread * jax.random.normal(stream_key, shape, jnp.float32)
    if cuts:
        drawn = drawn * block_scale(stream_key, shape, cuts, -0.22, 0.18)
    return jnp.clip(drawn, -most, most).astype(held_as)


def setup_inputs(seed: int = 0) -> dict:
    splits = jax.random.split(jax.random.key(seed), 18)
    residual_in = scatter_about(splits[0], (TOKENS, D), 1.0, 6.0, ((0, 32),))
    queries = scatter_about(splits[1], (TOKENS, OUTPUT_CHANNELS * DK), 1.0, 6.0, ((0, 32),))
    keys_in = scatter_about(splits[2], (TOKENS, OUTPUT_CHANNELS * DK), 1.0, 6.0, ((0, 32),))
    values_in = scatter_about(splits[3], (TOKENS, OUTPUT_CHANNELS * DV), 1.0, 6.0, ((0, 32),))
    out_gate = scatter_about(splits[4], (TOKENS, OUTPUT_CHANNELS * DV), 1.0, 6.0, ((0, 32),))
    log_decay = draw_log_decay(jax.random.fold_in(splits[17], 71), 0)
    beta_rate = jnp.clip(0.05 + 0.9 * jax.random.uniform(splits[6], (OUTPUT_CHANNELS, TOKENS), jnp.float32) ** block_scale(splits[6], (OUTPUT_CHANNELS, TOKENS), ((1, 32),), -0.2, 0.2), 0.05, 0.95)
    head_gain = jnp.clip(1.0 + 0.18 * jax.random.normal(splits[7], (DV,), jnp.float32), 0.1, 1.9)
    moe_gain = jnp.clip(1.0 + 0.18 * jax.random.normal(splits[8], (D,), jnp.float32), 0.1, 1.9)
    state_cache = scatter_about(splits[9], (SHARD_TOTAL, SLOTS, OUTPUT_CHANNELS, DK, DV), 0.3, 1.8, ((0, 32),), jnp.float32)
    hit_holder = touch_ends(ranked(splits[10], (SHARD_TOTAL,), HOLDERS, 2), jax.random.fold_in(splits[10], 3), 0, HOLDERS - 1).astype(jnp.int32)
    hit_slot = touch_ends(jax.random.randint(splits[11], (SHARD_TOTAL,), 0, SLOTS), jax.random.fold_in(splits[11], 1), 0, SLOTS - 1).astype(jnp.int32)
    expert_ids_keys = jax.random.split(jax.random.fold_in(splits[12], 1), TOKENS // SHARD_LENGTH)
    expert_ids_turns = jax.random.permutation(jax.random.fold_in(splits[12], 3), TOKENS // SHARD_LENGTH)
    expert_ids = jax.vmap(lambda own, number: deal_out(jax.random.fold_in(splits[12], 2), own, number, SHARD_LENGTH, EXPERTS, TOPK, MOST, 2))(expert_ids_keys, expert_ids_turns).reshape((TOKENS, TOPK))
    gate_weight = jnp.clip(jnp.exp(math.log(0.3) - 2.3025852 * jax.random.uniform(splits[13], (TOKENS, TOPK), jnp.float32) ** block_scale(splits[13], (TOKENS, TOPK), ((0, 32),), -0.2, 0.2)), 0.03, 0.3)
    w_gate = scatter_about(splits[14], (EXPERTS, D, FF), D ** -0.5, 0.125, ((0, 8),))
    w_up = scatter_about(splits[15], (EXPERTS, D, FF), D ** -0.5, 0.125, ((0, 8),))
    w_down = scatter_about(splits[16], (EXPERTS, FF, D), FF ** -0.5, 0.25, ((0, 8),))
    return dict(residual_in=residual_in, queries=queries, keys_in=keys_in, values_in=values_in, out_gate=out_gate, log_decay=log_decay, beta_rate=beta_rate, head_gain=head_gain, moe_gain=moe_gain, state_cache=state_cache, hit_holder=hit_holder, hit_slot=hit_slot, expert_ids=expert_ids, gate_weight=gate_weight, w_gate=w_gate, w_up=w_up, w_down=w_down)


TOP_PRECISION = lax.Precision.HIGHEST

def unit_rows(block):
    block = block.astype(jnp.float32)
    return block / jnp.sqrt(lax.optimization_barrier(jnp.sum(block * block, axis=-1, keepdims=True)) + 1e-06)

def reference(residual_in, queries, keys_in, values_in, out_gate, log_decay, beta_rate, head_gain, moe_gain, state_cache, hit_holder, hit_slot, expert_ids, gate_weight, w_gate, w_up, w_down):
    query_normalized = unit_rows(queries.reshape(SHARD_TOTAL, SHARD_LENGTH, OUTPUT_CHANNELS, DK)).transpose(1, 0, 2, 3)
    key_normalized = unit_rows(keys_in.reshape(SHARD_TOTAL, SHARD_LENGTH, OUTPUT_CHANNELS, DK)).transpose(1, 0, 2, 3)
    v_rows = values_in.reshape(SHARD_TOTAL, SHARD_LENGTH, OUTPUT_CHANNELS, DV).astype(jnp.float32).transpose(1, 0, 2, 3)
    decay = jnp.exp(log_decay).reshape(OUTPUT_CHANNELS, SHARD_TOTAL, SHARD_LENGTH).transpose(2, 1, 0)
    writes = beta_rate.reshape(OUTPUT_CHANNELS, SHARD_TOTAL, SHARD_LENGTH).transpose(2, 1, 0)
    blocks = jnp.arange(SHARD_TOTAL, dtype=jnp.int32)
    holder = (hit_holder * GROUP + blocks % GROUP).astype(jnp.int32)
    initial_state = state_cache[holder, hit_slot.astype(jnp.int32)]

    def advance(state, inputs):
        q_now, k_now, v_now, a_now, b_now = inputs
        k_read = jnp.einsum('chk,chkv->chv', k_now, state, precision=TOP_PRECISION)
        state = a_now[:, :, None, None] * (state - b_now[:, :, None, None] * k_now[:, :, :, None] * k_read[:, :, None, :])
        state = state + b_now[:, :, None, None] * k_now[:, :, :, None] * v_now[:, :, None, :]
        out_now = jnp.einsum('chk,chkv->chv', q_now, state, precision=TOP_PRECISION)
        return (state, out_now)
    final_state, outs = lax.scan(advance, initial_state, (query_normalized, key_normalized, v_rows, decay, writes))
    o_rows = outs.transpose(1, 0, 2, 3)
    scaled = o_rows / jnp.sqrt(lax.optimization_barrier(jnp.mean(o_rows * o_rows, axis=-1, keepdims=True)) + 1e-06) * head_gain
    gated = scaled * jax.nn.silu(out_gate.reshape(SHARD_TOTAL, SHARD_LENGTH, OUTPUT_CHANNELS, DV).astype(jnp.float32))
    mixer_out = (residual_in.astype(jnp.float32) + gated.reshape(TOKENS, D)).astype(jnp.bfloat16)
    mixer_f = mixer_out.astype(jnp.float32)
    moe_in = (mixer_f / jnp.sqrt(lax.optimization_barrier(jnp.mean(mixer_f * mixer_f, axis=-1, keepdims=True)) + 1e-06) * moe_gain).astype(jnp.bfloat16)
    padded = jnp.concatenate([moe_in, jnp.zeros((1, D), jnp.bfloat16)], axis=0)
    capacity = SHARD_TOTAL * MOST

    def one_expert(summed, expert):
        picked = expert_ids == expert
        weight = lax.optimization_barrier(jnp.sum(jnp.where(picked, gate_weight, jnp.float32(0.0)), axis=1))
        weight = jnp.concatenate([weight, jnp.zeros((1,), jnp.float32)])
        row_index = jnp.nonzero(jnp.any(picked, axis=1), size=capacity, fill_value=TOKENS)[0].astype(jnp.int32)
        chosen = padded[row_index]
        gate_part = jnp.dot(chosen, w_gate[expert], preferred_element_type=jnp.float32)
        up_part = jnp.dot(chosen, w_up[expert], preferred_element_type=jnp.float32)
        hidden_rows = (jax.nn.silu(gate_part) * up_part).astype(jnp.bfloat16)
        rounded = jnp.dot(hidden_rows, w_down[expert], preferred_element_type=jnp.float32).astype(jnp.bfloat16)
        rows_f = lax.optimization_barrier(rounded).astype(jnp.float32)
        summed = summed.at[row_index].add(weight[row_index][:, None] * rows_f)
        return (summed, None)
    summed, unused = lax.scan(one_expert, jnp.zeros((TOKENS + 1, D), jnp.float32), jnp.arange(EXPERTS, dtype=jnp.int32))
    expert_out = summed[:TOKENS].astype(jnp.bfloat16)
    return (mixer_out, expert_out, final_state)
```

```python
import jax
import jax.numpy as jnp
from jax import lax
from jax.experimental import pallas as pl
from jax.experimental.pallas import tpu as pltpu
from jax.sharding import PartitionSpec as P

MOST = 56
PAIR = 2 * MOST
EPS = 1e-06
HEADS_A_STEP = 4
STATE_CHUNKS = 4
RETURN_CHUNKS = 4
BF = jnp.bfloat16
F32 = jnp.float32
VMEM_BYTES = 60 * 1024 * 1024


def iota(shape, dim):
    return lax.broadcasted_iota(jnp.int32, shape, dim)


def mm(a, b):
    return jnp.dot(a, b, preferred_element_type=F32)


def silu(x):
    return x / (1.0 + jnp.exp(-x))


def prepare_kernel(q_ref, k_ref, lb_ref, lbt_ref, kq_ref, t_ref, mk_ref):
    rows = q_ref.shape[0]
    dk = 128
    at_row = iota((rows, rows), 0)
    at_col = iota((rows, rows), 1)
    strict = at_row > at_col
    inclusive = at_row >= at_col
    lower = inclusive.astype(F32)
    upper = (at_row <= at_col).astype(F32)
    top = lax.Precision.HIGHEST
    total_row = jnp.dot(lb_ref[0], upper, precision=top, preferred_element_type=F32)
    total_col = jnp.dot(lower, lbt_ref[0], precision=top, preferred_element_type=F32)
    solved = []
    mixes = []
    for i in range(HEADS_A_STEP):
        span = slice(i * dk, (i + 1) * dk)
        q = q_ref[:, span].astype(F32)
        k = k_ref[:, span].astype(F32)
        q = q / jnp.sqrt(jnp.sum(q * q, axis=-1, keepdims=True) + EPS)
        k = k / jnp.sqrt(jnp.sum(k * k, axis=-1, keepdims=True) + EPS)
        l_col = total_col[:, i : i + 1]
        l_row = total_row[i : i + 1, :]
        beta = lbt_ref[0][:, HEADS_A_STEP + i : HEADS_A_STEP + i + 1]
        ratio = jnp.where(inclusive, jnp.exp(jnp.where(inclusive, l_col - l_row, 0.0)), 0.0)
        kb = k.astype(BF)
        both = lax.dot_general(
            jnp.concatenate([kb, q.astype(BF)], axis=0),
            kb,
            (((1,), (1,)), ((), ())),
            preferred_element_type=F32,
        )
        mix = jnp.where(strict, beta * ratio * both[:rows], 0.0)
        growth = jnp.exp(l_col)
        trail = jnp.exp(l_col[rows - 1 : rows, :] - l_col)
        kq_ref[i] = jnp.concatenate([k * (beta * growth), q * growth], axis=0).astype(BF)
        mk_ref[i] = jnp.concatenate(
            [ratio * both[rows:], jnp.transpose(k * trail)], axis=0
        ).astype(BF)
        mixes.append(mix)
        first = (at_row // 2 == at_col // 2) & strict
        solved.append((at_row == at_col).astype(F32) - jnp.where(first, mix, 0.0))
    size = 2
    while size < rows:
        here = (
            (at_row // (2 * size) == at_col // (2 * size))
            & ((at_row // size) % 2 == 1)
            & ((at_col // size) % 2 == 0)
        )
        for i in range(HEADS_A_STEP):
            t = solved[i].astype(BF)
            block = jnp.where(here, mixes[i], 0.0).astype(BF)
            solved[i] = solved[i] - mm(t, mm(block, t).astype(BF))
        size *= 2
    for i in range(HEADS_A_STEP):
        t_ref[i] = solved[i].astype(BF)


def prepare(queries, keys_in, lb, lbt):
    rows = queries.shape[0]
    groups = lb.shape[0]
    heads = groups * HEADS_A_STEP
    wide = HEADS_A_STEP * 128
    return pl.pallas_call(
        prepare_kernel,
        grid=(groups,),
        in_specs=[
            pl.BlockSpec((rows, wide), lambda i: (0, i)),
            pl.BlockSpec((rows, wide), lambda i: (0, i)),
            pl.BlockSpec((1,) + lb.shape[1:], lambda i: (i, 0, 0)),
            pl.BlockSpec((1,) + lbt.shape[1:], lambda i: (i, 0, 0)),
        ],
        out_specs=[
            pl.BlockSpec((HEADS_A_STEP, 2 * rows, 128), lambda i: (i, 0, 0)),
            pl.BlockSpec((HEADS_A_STEP, rows, rows), lambda i: (i, 0, 0)),
            pl.BlockSpec((HEADS_A_STEP, rows + 128, rows), lambda i: (i, 0, 0)),
        ],
        out_shape=[
            jax.ShapeDtypeStruct((heads, 2 * rows, 128), BF),
            jax.ShapeDtypeStruct((heads, rows, rows), BF),
            jax.ShapeDtypeStruct((heads, rows + 128, rows), BF),
        ],
        compiler_params=pltpu.CompilerParams(vmem_limit_bytes=VMEM_BYTES),
        cost_estimate=pl.CostEstimate(flops=int(2e9), transcendentals=0, bytes_accessed=4000000),
        name="prepare",
    )(queries, keys_in, lb, lbt)


def resume_kernel(pick_ref, *refs, peers, first_head):
    cache_ref, got_refs, refs = refs[0], refs[1 : 1 + peers], refs[1 + peers :]
    kq_ref, t_ref, mk_ref, v_ref, lb_ref, lbt_ref, gate_ref, res_ref, gain_ref = refs[:9]
    out_ref, next_ref, own_buf, got_buf, sem_own, sem_got = refs[9:]
    heads, rows, _ = t_ref.shape
    place = pick_ref[0]
    slot = pick_ref[1]
    own = pltpu.make_async_copy(cache_ref.at[0, slot, pl.ds(first_head, heads)], own_buf, sem_own)
    own.start()
    for j in range(peers):

        @pl.when(place == j + 1)
        def _(j=j):
            copy = pltpu.make_async_copy(got_refs[j], got_buf, sem_got)
            copy.start()
            copy.wait()

    own.wait()
    here = place == 0
    for i in range(heads):
        span = slice(i * 128, (i + 1) * 128)
        state = jnp.where(here, own_buf[i], got_buf[i].astype(F32))
        beta = lbt_ref[0][:, HEADS_A_STEP + i : HEADS_A_STEP + i + 1]
        read = mm(kq_ref[i], state.astype(BF))
        rest = beta * v_ref[:, span].astype(F32) - read[:rows]
        fixed = mm(t_ref[i], rest.astype(BF)).astype(BF)
        added = mm(mk_ref[i], fixed)
        o = read[rows:] + added[:rows]
        last = jnp.exp(jnp.sum(lb_ref[0][i : i + 1, :], axis=-1, keepdims=True))
        next_ref[i] = last * state + added[rows:]
        scaled = o / jnp.sqrt(jnp.mean(o * o, axis=-1, keepdims=True) + EPS) * gain_ref[...]
        gated = scaled * silu(gate_ref[:, span].astype(F32))
        out_ref[:, span] = (res_ref[:, span].astype(F32) + gated).astype(BF)


def resume(pick, cache, got, kq, t, mk, values, lb, lbt, gate, residual, gain, group, heads):
    rows = values.shape[0]
    wide = heads * 128
    any_spec = pl.BlockSpec(memory_space=pl.ANY)
    cols = pl.BlockSpec((rows, wide), lambda i, p: (0, group))
    import_heads = lambda i, p: (group, 0, 0)
    return pl.pallas_call(
        lambda *refs: resume_kernel(*refs, peers=len(got), first_head=group * heads),
        grid_spec=pltpu.PrefetchScalarGridSpec(
            num_scalar_prefetch=1,
            grid=(1,),
            in_specs=[any_spec]
            + [any_spec] * len(got)
            + [
                pl.BlockSpec((heads,) + kq.shape[1:], import_heads),
                pl.BlockSpec((heads,) + t.shape[1:], import_heads),
                pl.BlockSpec((heads,) + mk.shape[1:], import_heads),
                cols,
                pl.BlockSpec((1,) + lb.shape[1:], import_heads),
                pl.BlockSpec((1,) + lbt.shape[1:], import_heads),
                cols,
                cols,
                pl.BlockSpec((1, 128), lambda i, p: (0, 0)),
            ],
            out_specs=[
                pl.BlockSpec((rows, wide), lambda i, p: (0, 0)),
                pl.BlockSpec((heads, 128, 128), lambda i, p: (0, 0, 0)),
            ],
            scratch_shapes=[
                pltpu.VMEM((heads, 128, 128), F32),
                pltpu.VMEM((heads, 128, 128), BF),
                pltpu.SemaphoreType.DMA,
                pltpu.SemaphoreType.DMA,
            ],
        ),
        out_shape=[
            jax.ShapeDtypeStruct((rows, wide), BF),
            jax.ShapeDtypeStruct((heads, 128, 128), F32),
        ],
        compiler_params=pltpu.CompilerParams(vmem_limit_bytes=VMEM_BYTES),
        cost_estimate=pl.CostEstimate(flops=int(1e9), transcendentals=0, bytes_accessed=3000000),
        name="resume",
    )(pick, cache, *got, kq, t, mk, values, lb, lbt, gate, residual, gain)


def hidden_kernel(*refs, blocks, parts, normed):
    count = 1 if normed else blocks * parts
    x_refs, refs = refs[:count], refs[count:]
    gain_ref, pos_ref, wt_ref, wg_ref, wu_ref, out_ref = refs[:6]
    if normed:
        all_ref = x_refs[0]
        chosen_ref = refs[6]
    else:
        all_ref, chosen_ref = refs[6:8]
        slab = 16

        @pl.when(pl.program_id(0) == 0)
        def _():
            gain = gain_ref[...]
            rows = x_refs[0].shape[0]
            for b in range(blocks):

                def step(s, carry, b=b):
                    at = pl.multiple_of(s * slab, slab)
                    x = jnp.concatenate(
                        [x_refs[b * parts + c][pl.ds(at, slab), :] for c in range(parts)], axis=1
                    ).astype(F32)
                    mean = jnp.mean(x * x, axis=-1, keepdims=True)
                    to = pl.multiple_of(b * rows + s * slab, slab)
                    all_ref[pl.ds(to, slab), :] = (x / jnp.sqrt(mean + EPS) * gain).astype(BF)
                    return carry

                lax.fori_loop(0, rows // slab, step, 0)

    pairs = pos_ref.shape[1]
    two = pos_ref.shape[3]
    weights = []
    for p in range(pairs):
        sel = iota((PAIR, two), 0) == pos_ref[0, p]
        weights.append(jnp.sum(jnp.where(sel, wt_ref[0, p], 0.0), axis=1, keepdims=True))
        chosen_ref[p * PAIR : (p + 1) * PAIR, :] = mm(
            sel.astype(F32).astype(BF), all_ref[p * two : (p + 1) * two, :]
        ).astype(BF)
    together = min(pairs, 4)
    for p in range(0, pairs, together):
        span = slice(p * PAIR, (p + together) * PAIR)
        x = chosen_ref[span, :]
        gate = mm(x, wg_ref[0])
        up = mm(x, wu_ref[0])
        weight = jnp.concatenate(weights[p : p + together], axis=0)
        out_ref[0, span, :] = (silu(gate) * up * weight).astype(BF)


def hidden(xs, parts, gain, pos, wt, w_gate, w_up, normed):
    experts, d, ff = w_gate.shape
    pairs, two = pos.shape[1], pos.shape[3]
    blocks = 2 * pairs
    one = pl.Buffered(1)
    scratch = [pltpu.VMEM((pairs * PAIR, d), BF)]
    if not normed:
        scratch = [pltpu.VMEM((pairs * two, d), BF)] + scratch
    return pl.pallas_call(
        lambda *refs: hidden_kernel(*refs, blocks=blocks, parts=parts, normed=normed),
        grid=(experts,),
        in_specs=[pl.BlockSpec(x.shape, lambda e: (0, 0), pipeline_mode=one) for x in xs]
        + [
            pl.BlockSpec((1, d), lambda e: (0, 0)),
            pl.BlockSpec((1, pairs, 1, two), lambda e: (e, 0, 0, 0)),
            pl.BlockSpec((1, pairs, 1, two), lambda e: (e, 0, 0, 0)),
            pl.BlockSpec((1, d, ff), lambda e: (e, 0, 0)),
            pl.BlockSpec((1, d, ff), lambda e: (e, 0, 0)),
        ],
        out_specs=pl.BlockSpec((1, pairs * PAIR, ff), lambda e: (e, 0, 0)),
        out_shape=jax.ShapeDtypeStruct((experts, pairs * PAIR, ff), BF),
        scratch_shapes=scratch,
        compiler_params=pltpu.CompilerParams(vmem_limit_bytes=VMEM_BYTES),
        cost_estimate=pl.CostEstimate(flops=int(9e9), transcendentals=0, bytes_accessed=24000000),
        name="hidden",
    )(*xs, gain, pos, wt, w_gate, w_up)


def down_kernel(pos_ref, h_ref, w_ref, own_ref, other_ref, sel_ref, rows_ref):
    experts = h_ref.shape[0]
    pairs, two, deep = sel_ref.shape
    half = two // 2

    @pl.when(pl.program_id(0) == 0)
    def _():
        lane = iota((two, deep), 1)
        for p in range(pairs):
            at = pos_ref[p * two : (p + 1) * two, :]
            hit = lane == at[:, 0:1]
            for e in range(1, experts):
                hit = hit | (lane == at[:, e : e + 1])
            sel_ref[p] = hit.astype(F32).astype(BF)

    for e in range(experts):
        rows = mm(h_ref[e], w_ref[e]).astype(BF)
        for p in range(pairs):
            rows_ref[p, e * PAIR : (e + 1) * PAIR, :] = rows[p * PAIR : (p + 1) * PAIR]
    for p in range(pairs):
        both = mm(sel_ref[p], rows_ref[p]).astype(BF)
        own_ref[p] = both[:half]
        other_ref[p] = both[half:]


def down(pos, h, w_down, chunk, chunks, two):
    experts, ff, d = w_down.shape
    pairs = h.shape[1] // PAIR
    wide = d // chunks
    tile = min(256, wide)
    steps = wide // tile
    out = jax.ShapeDtypeStruct((pairs, two // 2, wide), BF)
    out_spec = pl.BlockSpec((pairs, two // 2, tile), lambda n: (0, 0, n))
    return pl.pallas_call(
        down_kernel,
        grid=(steps,),
        in_specs=[
            pl.BlockSpec(pos.shape, lambda n: (0, 0)),
            pl.BlockSpec(h.shape, lambda n: (0, 0, 0)),
            pl.BlockSpec((experts, ff, tile), lambda n: (0, 0, chunk * steps + n)),
        ],
        out_specs=[out_spec, out_spec],
        out_shape=[out, out],
        scratch_shapes=[
            pltpu.VMEM((pairs, two, experts * PAIR), BF),
            pltpu.VMEM((pairs, experts * PAIR, tile), BF),
        ],
        compiler_params=pltpu.CompilerParams(vmem_limit_bytes=VMEM_BYTES),
        cost_estimate=pl.CostEstimate(
            flops=int(6e9) // chunks, transcendentals=0, bytes_accessed=12000000 // chunks
        ),
        name="down",
    )(pos, h, w_down)


def swap(x, axis, bits):
    size = lax.axis_size(axis)
    return lax.ppermute(x, axis, [(i, i ^ bits) for i in range(size)])


def local(
    residual_in,
    queries,
    keys_in,
    values_in,
    out_gate,
    log_decay,
    beta_rate,
    head_gain,
    moe_gain,
    state_cache,
    hit_holder,
    hit_slot,
    expert_ids,
    gate_weight,
    w_gate,
    w_up,
    w_down,
):
    rows, d = queries.shape
    head_count = log_decay.shape[0]
    holders = lax.axis_size("dp")
    group = lax.axis_size("expert")
    own_dp = lax.axis_index("dp")
    own_ep = lax.axis_index("expert")
    experts = w_gate.shape[0]
    pairs = group // 2
    heads = head_count // STATE_CHUNKS

    wish = jnp.concatenate([hit_holder, hit_slot])
    sends = []
    for j in range(1, holders):
        asked = swap(wish, "dp", j)
        sends.append(jnp.where(asked[0] == own_dp, asked[1], 0))
    got = []
    for g in range(STATE_CHUNKS):
        got.append([])
        for j in range(1, holders):
            piece = lax.dynamic_slice(
                state_cache, (0, sends[j - 1], g * heads, 0, 0), (1, 1, heads) + state_cache.shape[3:]
            )[0, 0].astype(BF)
            got[g].append(swap(piece, "dp", j))
    pick = jnp.stack([hit_holder[0] ^ own_dp, hit_slot[0]])

    all_experts = group * experts
    named = expert_ids.T[None] == jnp.arange(all_experts, dtype=jnp.int32)[:, None, None]
    dense = jnp.sum(jnp.where(named, gate_weight.T[None], 0.0), axis=1)
    spread = lax.all_gather(dense, "expert", axis=0).reshape(group, group, experts, rows)
    mine = lax.dynamic_index_in_dim(spread, own_ep, 1, False)
    order = jnp.arange(group, dtype=jnp.int32) ^ own_ep
    mine = mine[order]
    routed = mine > 0.0
    before = jnp.arange(rows)[:, None] < jnp.arange(rows)[None, :]
    rank = jnp.dot(
        routed.astype(F32).reshape(group * experts, rows), before.astype(F32)
    ).reshape(group, experts, rows)
    rank = rank.astype(jnp.int32) + (jnp.arange(group, dtype=jnp.int32) % 2 * MOST)[:, None, None]
    rank = jnp.where(routed, rank, -100000)
    pos_row = rank.transpose(1, 0, 2).reshape(experts, pairs, 1, 2 * rows)
    wt_row = mine.transpose(1, 0, 2).reshape(experts, pairs, 1, 2 * rows)
    pos_col = rank.transpose(0, 2, 1).reshape(group * rows, experts)
    pos_col = pos_col + jnp.arange(experts, dtype=jnp.int32)[None, :] * PAIR

    groups = head_count // HEADS_A_STEP
    lb = jnp.concatenate(
        [
            log_decay.reshape(groups, HEADS_A_STEP, rows),
            beta_rate.reshape(groups, HEADS_A_STEP, rows),
        ],
        axis=1,
    )
    lbt = lb.transpose(0, 2, 1)
    kq, t, mk = prepare(queries, keys_in, lb, lbt)
    mixed, states = [], []
    for g in range(STATE_CHUNKS):
        m, s = resume(
            pick, state_cache, got[g], kq, t, mk, values_in, lb, lbt, out_gate, residual_in,
            head_gain[None], g, heads,
        )
        mixed.append(m)
        states.append(s)

    mixer_out = jnp.concatenate(mixed, axis=1)

    gain = moe_gain[None]
    outs = []
    if group <= 8:
        blocks = [[None] * STATE_CHUNKS for _ in range(group)]
        for c in range(STATE_CHUNKS):
            for r in range(pairs):
                near = mixed[c] if r == 0 else swap(mixed[c], "expert", 2 * r)
                blocks[2 * r][c] = near
                blocks[2 * r + 1][c] = swap(near, "expert", 1)
        xs = [blocks[b][c] for b in range(group) for c in range(STATE_CHUNKS)]
        h = hidden(xs, STATE_CHUNKS, gain, pos_row, wt_row, w_gate, w_up, False)
        for c in range(RETURN_CHUNKS):
            own, other = down(pos_col, h, w_down, c, RETURN_CHUNKS, 2 * rows)
            came = swap(other, "expert", 1)
            total = own[0].astype(F32) + came[0].astype(F32)
            for r in range(1, pairs):
                chip = (own[r].astype(F32) + came[r].astype(F32)).astype(BF)
                total = total + swap(chip, "expert", 2 * r).astype(F32)
            outs.append(total.astype(BF))
    else:
        x = lax.all_gather(mixer_out, "expert", axis=0)[order].reshape(group * rows, d).astype(F32)
        x = (x / jnp.sqrt(jnp.mean(x * x, axis=-1, keepdims=True) + EPS) * gain).astype(BF)
        h = hidden([x], 1, gain, pos_row, wt_row, w_gate, w_up, True)
        for c in range(RETURN_CHUNKS):
            own, other = down(pos_col, h, w_down, c, RETURN_CHUNKS, 2 * rows)
            part = jnp.stack([own, other], axis=1).reshape(group, rows, -1)[order]
            outs.append(lax.psum_scatter(part, "expert", scatter_dimension=0))
    expert_out = jnp.concatenate(outs, axis=1)
    return (mixer_out, expert_out, jnp.concatenate(states, axis=0)[None])


def solution(mesh):
    both = ("dp", "expert")
    rows = P(both, None)
    placed = (
        rows,
        rows,
        rows,
        rows,
        rows,
        P(None, both),
        P(None, both),
        P(),
        P(),
        P(both, None, None, None, None),
        P(both),
        P(both),
        rows,
        rows,
        P("expert", None, None),
        P("expert", None, None),
        P("expert", None, None),
    )
    return jax.shard_map(
        local,
        mesh=mesh,
        in_specs=placed,
        out_specs=(rows, rows, P(both, None, None, None)),
        check_vma=False,
    )
```

```python
import jax
import jax.numpy as jnp
from jax import lax
from jax.experimental import pallas as pl
from jax.experimental.pallas import tpu as pltpu
from jax.sharding import PartitionSpec as P

MOST = 56
PAIR = 2 * MOST
EPS = 1e-06
HEADS_A_STEP = 4
HEAD_CHUNKS = (8, 8)
STAGES = ((0, 1), (2,), (3,))
LANES = 128
FAR = -100000.0
BF = jnp.bfloat16
F32 = jnp.float32
VMEM_BYTES = 60 * 1024 * 1024


def iota(shape, dim):
    return lax.broadcasted_iota(jnp.int32, shape, dim)


def mm(a, b):
    return jnp.dot(a, b, preferred_element_type=F32)


def silu(x):
    return x / (1.0 + jnp.exp(-x))


def prepare_kernel(q_ref, k_ref, lb_ref, lbt_ref, kq_ref, t_ref, mk_ref):
    rows = q_ref.shape[0]
    dk = 128
    at_row = iota((rows, rows), 0)
    at_col = iota((rows, rows), 1)
    strict = at_row > at_col
    inclusive = at_row >= at_col
    lower = inclusive.astype(F32)
    upper = (at_row <= at_col).astype(F32)
    top = lax.Precision.HIGHEST
    total_row = jnp.dot(lb_ref[0], upper, precision=top, preferred_element_type=F32)
    total_col = jnp.dot(lower, lbt_ref[0], precision=top, preferred_element_type=F32)
    solved = []
    mixes = []
    for i in range(HEADS_A_STEP):
        span = slice(i * dk, (i + 1) * dk)
        q = q_ref[:, span].astype(F32)
        k = k_ref[:, span].astype(F32)
        q = q / jnp.sqrt(jnp.sum(q * q, axis=-1, keepdims=True) + EPS)
        k = k / jnp.sqrt(jnp.sum(k * k, axis=-1, keepdims=True) + EPS)
        l_col = total_col[:, i : i + 1]
        l_row = total_row[i : i + 1, :]
        beta = lbt_ref[0][:, HEADS_A_STEP + i : HEADS_A_STEP + i + 1]
        ratio = jnp.where(inclusive, jnp.exp(jnp.where(inclusive, l_col - l_row, 0.0)), 0.0)
        kb = k.astype(BF)
        both = lax.dot_general(
            jnp.concatenate([kb, q.astype(BF)], axis=0),
            kb,
            (((1,), (1,)), ((), ())),
            preferred_element_type=F32,
        )
        mix = jnp.where(strict, beta * ratio * both[:rows], 0.0)
        growth = jnp.exp(l_col)
        trail = jnp.exp(l_col[rows - 1 : rows, :] - l_col)
        kq_ref[i] = jnp.concatenate([k * (beta * growth), q * growth], axis=0).astype(BF)
        mk_ref[i] = jnp.concatenate(
            [ratio * both[rows:], jnp.transpose(k * trail)], axis=0
        ).astype(BF)
        mixes.append(mix)
        first = (at_row // 2 == at_col // 2) & strict
        solved.append((at_row == at_col).astype(F32) - jnp.where(first, mix, 0.0))
    size = 2
    while size < rows:
        here = (
            (at_row // (2 * size) == at_col // (2 * size))
            & ((at_row // size) % 2 == 1)
            & ((at_col // size) % 2 == 0)
        )
        for i in range(HEADS_A_STEP):
            t = solved[i].astype(BF)
            block = jnp.where(here, mixes[i], 0.0).astype(BF)
            solved[i] = solved[i] - mm(t, mm(block, t).astype(BF))
        size *= 2
    for i in range(HEADS_A_STEP):
        t_ref[i] = solved[i].astype(BF)


def prepare(queries, keys_in, lb, lbt):
    rows = queries.shape[0]
    groups = lb.shape[0]
    heads = groups * HEADS_A_STEP
    wide = HEADS_A_STEP * 128
    return pl.pallas_call(
        prepare_kernel,
        grid=(groups,),
        in_specs=[
            pl.BlockSpec((rows, wide), lambda i: (0, i)),
            pl.BlockSpec((rows, wide), lambda i: (0, i)),
            pl.BlockSpec((1,) + lb.shape[1:], lambda i: (i, 0, 0)),
            pl.BlockSpec((1,) + lbt.shape[1:], lambda i: (i, 0, 0)),
        ],
        out_specs=[
            pl.BlockSpec((HEADS_A_STEP, 2 * rows, 128), lambda i: (i, 0, 0)),
            pl.BlockSpec((HEADS_A_STEP, rows, rows), lambda i: (i, 0, 0)),
            pl.BlockSpec((HEADS_A_STEP, rows + 128, rows), lambda i: (i, 0, 0)),
        ],
        out_shape=[
            jax.ShapeDtypeStruct((heads, 2 * rows, 128), BF),
            jax.ShapeDtypeStruct((heads, rows, rows), BF),
            jax.ShapeDtypeStruct((heads, rows + 128, rows), BF),
        ],
        compiler_params=pltpu.CompilerParams(vmem_limit_bytes=VMEM_BYTES),
        cost_estimate=pl.CostEstimate(flops=int(2e9), transcendentals=0, bytes_accessed=4000000),
        name="prepare",
    )(queries, keys_in, lb, lbt)


def resume_kernel(pick_ref, *refs, peers, first_head, experts):
    cache_ref, got_refs, refs = refs[0], refs[1 : 1 + peers], refs[1 + peers :]
    kq_ref, t_ref, mk_ref, v_ref, lb_ref, lbt_ref, gate_ref, res_ref, gain_ref = refs[:9]
    ids_ref, weight_ref = refs[9:11]
    out_ref, next_ref, own_buf, got_buf, sem_own, sem_got = refs[11:]
    heads, rows, _ = t_ref.shape
    steps = own_buf.shape[0] // heads
    at = pl.program_id(0)
    place = pick_ref[0]
    slot = pick_ref[1]

    def own_copy(s):
        return pltpu.make_async_copy(
            cache_ref.at[0, slot, pl.ds(first_head + s * heads, heads)],
            own_buf.at[pl.ds(s * heads, heads)],
            sem_own.at[s],
        )

    def got_copy(s, j):
        return pltpu.make_async_copy(
            got_refs[j].at[pl.ds(s * heads, heads)],
            got_buf.at[pl.ds(s * heads, heads)],
            sem_got.at[s],
        )

    @pl.when(at == 0)
    def _():
        for s in range(steps):
            own_copy(s).start()
            for j in range(peers):

                @pl.when(place == j + 1)
                def _(s=s, j=j):
                    got_copy(s, j).start()

        if experts:
            lane = iota((rows, LANES), 1)
            named = jnp.zeros((rows, LANES), F32)
            for k in range(ids_ref.shape[1]):
                hit = lane % experts == ids_ref[:, k : k + 1]
                named = jnp.where(hit, weight_ref[:, k : k + 1], named)
            coarse = named.astype(BF)
            fine = named - coarse.astype(F32)
            both = jnp.where(lane < experts, coarse.astype(F32), fine)
            both = jnp.where(lane < 2 * experts, both, 0.0)
            out_ref[:, out_ref.shape[1] - LANES :] = both.astype(BF)

    own_copy(at).wait()

    @pl.when(place > 0)
    def _():
        got_copy(at, 0).wait()

    here = place == 0
    for i in range(heads):
        span = slice(i * 128, (i + 1) * 128)
        head = at * heads + i
        state = jnp.where(here, own_buf[head], got_buf[head].astype(F32))
        beta = lbt_ref[0][:, HEADS_A_STEP + i : HEADS_A_STEP + i + 1]
        read = mm(kq_ref[i], state.astype(BF))
        rest = beta * v_ref[:, span].astype(F32) - read[:rows]
        fixed = mm(t_ref[i], rest.astype(BF)).astype(BF)
        added = mm(mk_ref[i], fixed)
        o = read[rows:] + added[:rows]
        last = jnp.exp(jnp.sum(lb_ref[0][i : i + 1, :], axis=-1, keepdims=True))
        next_ref[i] = last * state + added[rows:]
        scaled = o / jnp.sqrt(jnp.mean(o * o, axis=-1, keepdims=True) + EPS) * gain_ref[...]
        gated = scaled * silu(gate_ref[:, span].astype(F32))
        mixed = (res_ref[:, span].astype(F32) + gated).astype(BF)
        out_ref[:, pl.ds(pl.multiple_of(head * 128, 128), 128)] = mixed


def resume(
    pick, cache, got, kq, t, mk, values, lb, lbt, gate, residual, gain, ids, weight, first, heads,
    experts,
):
    rows = values.shape[0]
    step = HEADS_A_STEP
    wide = heads * 128 + (LANES if experts else 0)
    base = first // step
    any_spec = pl.BlockSpec(memory_space=pl.ANY)
    cols = pl.BlockSpec((rows, step * 128), lambda i, p: (0, base + i))
    group = lambda i, p: (base + i, 0, 0)
    whole = lambda i, p: (0, 0)
    return pl.pallas_call(
        lambda *refs: resume_kernel(*refs, peers=len(got), first_head=first, experts=experts),
        grid_spec=pltpu.PrefetchScalarGridSpec(
            num_scalar_prefetch=1,
            grid=(heads // step,),
            in_specs=[any_spec]
            + [any_spec] * len(got)
            + [
                pl.BlockSpec((step,) + kq.shape[1:], group),
                pl.BlockSpec((step,) + t.shape[1:], group),
                pl.BlockSpec((step,) + mk.shape[1:], group),
                cols,
                pl.BlockSpec((1,) + lb.shape[1:], group),
                pl.BlockSpec((1,) + lbt.shape[1:], group),
                cols,
                cols,
                pl.BlockSpec((1, 128), whole),
                pl.BlockSpec(ids.shape, whole),
                pl.BlockSpec(weight.shape, whole),
            ],
            out_specs=[
                pl.BlockSpec((rows, wide), whole),
                pl.BlockSpec((step, 128, 128), lambda i, p: (i, 0, 0)),
            ],
            scratch_shapes=[
                pltpu.VMEM((heads, 128, 128), F32),
                pltpu.VMEM((heads, 128, 128), BF),
                pltpu.SemaphoreType.DMA((heads // step,)),
                pltpu.SemaphoreType.DMA((heads // step,)),
            ],
        ),
        out_shape=[
            jax.ShapeDtypeStruct((rows, wide), BF),
            jax.ShapeDtypeStruct((heads, 128, 128), F32),
        ],
        compiler_params=pltpu.CompilerParams(vmem_limit_bytes=VMEM_BYTES),
        cost_estimate=pl.CostEstimate(flops=int(1e9), transcendentals=0, bytes_accessed=6000000),
        name="resume",
    )(pick, cache, *got, kq, t, mk, values, lb, lbt, gate, residual, gain, ids, weight)


def expert_kernel(first_ref, *refs, blocks, parts, experts, all_experts, halves):
    x_refs, refs = refs[: blocks * parts], refs[blocks * parts :]
    gain_ref, wg_ref, wu_ref, wd_ref, own_ref, other_ref = refs[:6]
    xs_ref, posr_ref, posc_ref, wr_ref, chosen_ref, slot_ref, acc_ref, rows_ref = refs[6:]
    step = pl.program_id(0)
    e = step // halves
    f = step % halves
    rows = x_refs[0].shape[0]
    d = xs_ref.shape[1]
    pairs = blocks // 2
    two = 2 * rows

    @pl.when(step == 0)
    def _():
        gain = gain_ref[...]
        slab = 16
        a, b = iota((LANES, LANES), 0), iota((LANES, LANES), 1)
        first = first_ref[0]
        mine = ((a == first + b) | (a == first + b + all_experts)) & (b < experts)
        mine = mine.astype(F32).astype(BF)
        before = (iota((rows, rows), 0) > iota((rows, rows), 1)).astype(F32).astype(BF)
        for n in range(blocks):
            last = x_refs[n * parts + parts - 1]
            weight = mm(last[:, last.shape[1] - LANES :], mine)
            routed = weight > 0.0
            rank = mm(before, routed.astype(F32).astype(BF)) + float(n % 2 * MOST)
            rank = jnp.where(routed, rank, FAR)
            posc_ref[n] = rank
            posr_ref[n] = jnp.transpose(rank)
            wr_ref[n] = jnp.transpose(weight)

            def norm(s, carry, n=n):
                at = pl.multiple_of(s * slab, slab)
                pieces = [x_refs[n * parts + c][pl.ds(at, slab), :] for c in range(parts)]
                pieces[-1] = pieces[-1][:, : pieces[-1].shape[1] - LANES]
                x = jnp.concatenate(pieces, axis=1).astype(F32)
                mean = jnp.mean(x * x, axis=-1, keepdims=True)
                to = pl.multiple_of(n * rows + s * slab, slab)
                xs_ref[pl.ds(to, slab), :] = (x / jnp.sqrt(mean + EPS) * gain).astype(BF)
                return carry

            lax.fori_loop(0, rows // slab, norm, 0, unroll=2)

    @pl.when(f == 0)
    def _():
        for p in range(pairs):
            pos = [posr_ref[2 * p + c, pl.ds(e, 1), :] for c in range(2)]
            weight = [wr_ref[2 * p + c, pl.ds(e, 1), :] for c in range(2)]
            sel = iota((PAIR, two), 0).astype(F32) == jnp.concatenate(pos, axis=1)
            span = slice(p * PAIR, (p + 1) * PAIR)
            slot_ref[span, :] = jnp.broadcast_to(
                jnp.sum(
                    jnp.where(sel, jnp.concatenate(weight, axis=1), 0.0), axis=1, keepdims=True
                ),
                (PAIR, LANES),
            )
            chosen_ref[span, :] = mm(
                sel.astype(F32).astype(BF), xs_ref[p * two : (p + 1) * two, :]
            ).astype(BF)

    x = chosen_ref[...]
    hidden = silu(mm(x, wg_ref[0])) * mm(x, wu_ref[0]) * slot_ref[:, 0:1]
    part = mm(hidden.astype(BF), wd_ref[0])

    @pl.when(f == 0)
    def _():
        acc_ref[...] = part

    @pl.when(f == halves - 1)
    def _():
        done = (part if halves == 1 else acc_ref[...] + part).astype(BF)
        to = pl.multiple_of(e * PAIR, 16)
        for p in range(pairs):
            rows_ref[p, pl.ds(to, PAIR), :] = done[p * PAIR : (p + 1) * PAIR]

    @pl.when(step == pl.num_programs(0) - 1)
    def _():
        lane = iota((two, experts * PAIR), 1).astype(F32)
        for p in range(pairs):
            at = jnp.concatenate([posc_ref[2 * p], posc_ref[2 * p + 1]], axis=0)
            hit = lane == at[:, 0:1]
            for n in range(1, experts):
                hit = hit | (lane == at[:, n : n + 1] + float(n * PAIR))
            both = mm(hit.astype(F32).astype(BF), rows_ref[p]).astype(BF)
            own_ref[p] = both[:rows]
            other_ref[p] = both[rows:]


def expert_stage(first, xs, parts, gain, w_gate, w_up, w_down, all_experts):
    experts, d, ff = w_gate.shape
    rows = xs[0].shape[0]
    blocks = len(xs) // parts
    pairs = blocks // 2
    halves = 2
    part = ff // halves
    one = pl.Buffered(1)
    out = jax.ShapeDtypeStruct((pairs, rows, d), BF)
    whole3 = lambda s, m: (0, 0, 0)
    return pl.pallas_call(
        lambda *refs: expert_kernel(
            *refs, blocks=blocks, parts=parts, experts=experts, all_experts=all_experts,
            halves=halves,
        ),
        grid_spec=pltpu.PrefetchScalarGridSpec(
            num_scalar_prefetch=1,
            grid=(experts * halves,),
            in_specs=[pl.BlockSpec(x.shape, lambda s, m: (0, 0), pipeline_mode=one) for x in xs]
            + [
                pl.BlockSpec((1, d), lambda s, m: (0, 0)),
                pl.BlockSpec((1, d, part), lambda s, m: (s // halves, 0, s % halves)),
                pl.BlockSpec((1, d, part), lambda s, m: (s // halves, 0, s % halves)),
                pl.BlockSpec((1, part, d), lambda s, m: (s // halves, s % halves, 0)),
            ],
            out_specs=[pl.BlockSpec(out.shape, whole3), pl.BlockSpec(out.shape, whole3)],
            scratch_shapes=[
                pltpu.VMEM((blocks * rows, d), BF),
                pltpu.VMEM((blocks, LANES, rows), F32),
                pltpu.VMEM((blocks, rows, LANES), F32),
                pltpu.VMEM((blocks, LANES, rows), F32),
                pltpu.VMEM((pairs * PAIR, d), BF),
                pltpu.VMEM((pairs * PAIR, LANES), F32),
                pltpu.VMEM((pairs * PAIR, d), F32),
                pltpu.VMEM((pairs, experts * PAIR, d), BF),
            ],
        ),
        out_shape=[out, out],
        compiler_params=pltpu.CompilerParams(vmem_limit_bytes=VMEM_BYTES),
        cost_estimate=pl.CostEstimate(
            flops=int(4e9) * pairs, transcendentals=0, bytes_accessed=30000000
        ),
        name="experts",
    )(first, *xs, gain, w_gate, w_up, w_down)


def swap(x, axis, bits):
    size = lax.axis_size(axis)
    return lax.ppermute(x, axis, [(i, i ^ bits) for i in range(size)])


def local(
    residual_in,
    queries,
    keys_in,
    values_in,
    out_gate,
    log_decay,
    beta_rate,
    head_gain,
    moe_gain,
    state_cache,
    hit_holder,
    hit_slot,
    expert_ids,
    gate_weight,
    w_gate,
    w_up,
    w_down,
):
    rows, d = queries.shape
    head_count = log_decay.shape[0]
    holders = lax.axis_size("dp")
    group = lax.axis_size("expert")
    own_dp = lax.axis_index("dp")
    own_ep = lax.axis_index("expert")
    experts = w_gate.shape[0]
    pairs = group // 2
    all_experts = group * experts
    chunks = HEAD_CHUNKS
    starts = [sum(chunks[:g]) for g in range(len(chunks))]

    wish = jnp.concatenate([hit_holder, hit_slot])
    sends = []
    for j in range(1, holders):
        asked = swap(wish, "dp", j)
        sends.append(jnp.where(asked[0] == own_dp, asked[1], 0))
    got = []
    for first, heads in zip(starts, chunks):
        got.append([])
        for j in range(1, holders):
            piece = lax.dynamic_slice(
                state_cache, (0, sends[j - 1], first, 0, 0), (1, 1, heads) + state_cache.shape[3:]
            )[0, 0].astype(BF)
            got[-1].append(swap(piece, "dp", j))
    pick = jnp.stack([hit_holder[0] ^ own_dp, hit_slot[0]])

    groups = head_count // HEADS_A_STEP
    lb = jnp.concatenate(
        [
            log_decay.reshape(groups, HEADS_A_STEP, rows),
            beta_rate.reshape(groups, HEADS_A_STEP, rows),
        ],
        axis=1,
    )
    lbt = lb.transpose(0, 2, 1)
    kq, t, mk = prepare(queries, keys_in, lb, lbt)
    mixed, states = [], []
    for g, (first, heads) in enumerate(zip(starts, chunks)):
        last = g == len(chunks) - 1
        m, s = resume(
            pick, state_cache, got[g], kq, t, mk, values_in, lb, lbt, out_gate, residual_in,
            head_gain[None], expert_ids, gate_weight, first, heads, all_experts if last else 0,
        )
        mixed.append(m)
        states.append(s)
    parts = len(chunks)
    mixer_out = jnp.concatenate(mixed[:-1] + [mixed[-1][:, :-LANES]], axis=1)

    gain = moe_gain[None]
    first_expert = (own_ep * experts)[None].astype(jnp.int32)
    weights = (w_gate, w_up, w_down)
    if group == 8:
        blocks = [[] for _ in range(group)]
        for c in range(parts):
            for r in (0, 2, 3, 1):
                near = mixed[c] if r == 0 else swap(mixed[c], "expert", 2 * r)
                blocks[2 * r].append(near)
                blocks[2 * r + 1].append(swap(near, "expert", 1))
        total = None
        for stage in STAGES:
            xs = [x for r in stage for x in blocks[2 * r] + blocks[2 * r + 1]]
            own, other = expert_stage(first_expert, xs, parts, gain, *weights, all_experts)
            came = swap(other, "expert", 1)
            for i, r in enumerate(stage):
                chip = own[i].astype(F32) + came[i].astype(F32)
                if r:
                    chip = swap(chip.astype(BF), "expert", 2 * r).astype(F32)
                total = chip if total is None else total + chip
        expert_out = total.astype(BF)
    else:
        order = jnp.arange(group, dtype=jnp.int32) ^ own_ep
        x = lax.all_gather(jnp.concatenate(mixed, axis=1), "expert", axis=0)[order]
        sums = []
        for p in range(0, group, 8):
            xs = [x[p + i] for i in range(8)]
            own, other = expert_stage(first_expert, xs, 1, gain, *weights, all_experts)
            sums.append(jnp.stack([own, other], axis=1).reshape(8, rows, d))
        part = jnp.concatenate(sums, axis=0)[order]
        expert_out = lax.psum_scatter(part, "expert", scatter_dimension=0)
    return (mixer_out, expert_out, jnp.concatenate(states, axis=0)[None])


def solution(mesh):
    both = ("dp", "expert")
    rows = P(both, None)
    placed = (
        rows,
        rows,
        rows,
        rows,
        rows,
        P(None, both),
        P(None, both),
        P(),
        P(),
        P(both, None, None, None, None),
        P(both),
        P(both),
        rows,
        rows,
        P("expert", None, None),
        P("expert", None, None),
        P("expert", None, None),
    )
    return jax.shard_map(
        local,
        mesh=mesh,
        in_specs=placed,
        out_specs=(rows, rows, P(both, None, None, None)),
        check_vma=False,
    )
```

```python
import jax
import jax.numpy as jnp
from jax import lax
from jax.experimental import pallas as pl
from jax.experimental.pallas import tpu as pltpu
from jax.sharding import PartitionSpec as P

MOST = 56
PAIR = 2 * MOST
EPS = 1e-06
HEADS_A_STEP = 4
HEAD_CHUNKS = (8, 8)
STAGES = ((0,), (1, 2), (3,))
PIECES = (1, 2, 4)
LANES = 128
FAR = -100000.0
BF = jnp.bfloat16
F32 = jnp.float32
VMEM_BYTES = 24 * 1024 * 1024


def iota(shape, dim):
    return lax.broadcasted_iota(jnp.int32, shape, dim)


def mm(a, b):
    return jnp.dot(a, b, preferred_element_type=F32)


def silu(x):
    return x / (1.0 + jnp.exp(-x))


def prepare_kernel(q_ref, k_ref, lb_ref, lbt_ref, kq_ref, t_ref, mk_ref):
    rows = q_ref.shape[0]
    dk = 128
    at_row = iota((rows, rows), 0)
    at_col = iota((rows, rows), 1)
    strict = at_row > at_col
    inclusive = at_row >= at_col
    lower = inclusive.astype(F32)
    upper = (at_row <= at_col).astype(F32)
    top = lax.Precision.HIGHEST
    total_row = jnp.dot(lb_ref[0], upper, precision=top, preferred_element_type=F32)
    total_col = jnp.dot(lower, lbt_ref[0], precision=top, preferred_element_type=F32)
    solved = []
    mixes = []
    for i in range(HEADS_A_STEP):
        span = slice(i * dk, (i + 1) * dk)
        q = q_ref[:, span].astype(F32)
        k = k_ref[:, span].astype(F32)
        q = q / jnp.sqrt(jnp.sum(q * q, axis=-1, keepdims=True) + EPS)
        k = k / jnp.sqrt(jnp.sum(k * k, axis=-1, keepdims=True) + EPS)
        l_col = total_col[:, i : i + 1]
        l_row = total_row[i : i + 1, :]
        beta = lbt_ref[0][:, HEADS_A_STEP + i : HEADS_A_STEP + i + 1]
        ratio = jnp.where(inclusive, jnp.exp(jnp.where(inclusive, l_col - l_row, 0.0)), 0.0)
        kb = k.astype(BF)
        both = lax.dot_general(
            jnp.concatenate([kb, q.astype(BF)], axis=0),
            kb,
            (((1,), (1,)), ((), ())),
            preferred_element_type=F32,
        )
        mix = jnp.where(strict, beta * ratio * both[:rows], 0.0)
        growth = jnp.exp(l_col)
        trail = jnp.exp(l_col[rows - 1 : rows, :] - l_col)
        kq_ref[i] = jnp.concatenate([k * (beta * growth), q * growth], axis=0).astype(BF)
        mk_ref[i] = jnp.concatenate(
            [ratio * both[rows:], jnp.transpose(k * trail)], axis=0
        ).astype(BF)
        mixes.append(mix)
        first = (at_row // 2 == at_col // 2) & strict
        solved.append((at_row == at_col).astype(F32) - jnp.where(first, mix, 0.0))
    size = 2
    while size < rows:
        here = (
            (at_row // (2 * size) == at_col // (2 * size))
            & ((at_row // size) % 2 == 1)
            & ((at_col // size) % 2 == 0)
        )
        for i in range(HEADS_A_STEP):
            t = solved[i].astype(BF)
            block = jnp.where(here, mixes[i], 0.0).astype(BF)
            solved[i] = solved[i] - mm(t, mm(block, t).astype(BF))
        size *= 2
    for i in range(HEADS_A_STEP):
        t_ref[i] = solved[i].astype(BF)


def prepare(queries, keys_in, lb, lbt, first, heads):
    rows = queries.shape[0]
    groups = heads // HEADS_A_STEP
    base = first // HEADS_A_STEP
    wide = HEADS_A_STEP * 128
    return pl.pallas_call(
        prepare_kernel,
        grid=(groups,),
        in_specs=[
            pl.BlockSpec((rows, wide), lambda i: (0, base + i)),
            pl.BlockSpec((rows, wide), lambda i: (0, base + i)),
            pl.BlockSpec((1,) + lb.shape[1:], lambda i: (base + i, 0, 0)),
            pl.BlockSpec((1,) + lbt.shape[1:], lambda i: (base + i, 0, 0)),
        ],
        out_specs=[
            pl.BlockSpec((HEADS_A_STEP, 2 * rows, 128), lambda i: (i, 0, 0)),
            pl.BlockSpec((HEADS_A_STEP, rows, rows), lambda i: (i, 0, 0)),
            pl.BlockSpec((HEADS_A_STEP, rows + 128, rows), lambda i: (i, 0, 0)),
        ],
        out_shape=[
            jax.ShapeDtypeStruct((heads, 2 * rows, 128), BF),
            jax.ShapeDtypeStruct((heads, rows, rows), BF),
            jax.ShapeDtypeStruct((heads, rows + 128, rows), BF),
        ],
        compiler_params=pltpu.CompilerParams(vmem_limit_bytes=VMEM_BYTES),
        cost_estimate=pl.CostEstimate(flops=1000, transcendentals=0, bytes_accessed=1000),
        name="prepare",
    )(queries, keys_in, lb, lbt)


def pack_kernel(own_ref, *refs, peers, first):
    asked, cache_ref, outs = refs[:peers], refs[peers], refs[peers + 1 : 2 * peers + 1]
    buf, sems = refs[2 * peers + 1 :]
    heads = buf.shape[1]
    copies = []
    for j in range(peers):
        slot = jnp.where(asked[j][0] == own_ref[0], asked[j][1], 0)
        copies.append(
            pltpu.make_async_copy(
                cache_ref.at[0, slot, pl.ds(first, heads)], buf.at[j], sems.at[j]
            )
        )
        copies[-1].start()
    for j in range(peers):
        copies[j].wait()
        outs[j][...] = buf[j].astype(BF)


def pack(own, asked, cache, first, heads):
    peers = len(asked)
    shape = (heads,) + cache.shape[3:]
    return pl.pallas_call(
        lambda *refs: pack_kernel(*refs, peers=peers, first=first),
        grid_spec=pltpu.PrefetchScalarGridSpec(
            num_scalar_prefetch=1 + peers,
            grid=(1,),
            in_specs=[pl.BlockSpec(memory_space=pl.ANY)],
            out_specs=[pl.BlockSpec(shape, lambda i, *p: (0, 0, 0))] * peers,
            scratch_shapes=[
                pltpu.VMEM((peers,) + shape, F32),
                pltpu.SemaphoreType.DMA((peers,)),
            ],
        ),
        out_shape=[jax.ShapeDtypeStruct(shape, BF)] * peers,
        compiler_params=pltpu.CompilerParams(vmem_limit_bytes=VMEM_BYTES),
        cost_estimate=pl.CostEstimate(flops=1000, transcendentals=0, bytes_accessed=1000),
        name="pack",
    )(own, *asked, cache)


def resume_kernel(pick_ref, *refs, peers, first_head, experts):
    cache_ref, got_refs, refs = refs[0], refs[1 : 1 + peers], refs[1 + peers :]
    kq_ref, t_ref, mk_ref, v_ref, lb_ref, lbt_ref, gate_ref, res_ref, gain_ref = refs[:9]
    ids_ref, weight_ref = refs[9:11]
    out_ref, next_ref, own_buf, got_buf, sem_own, sem_got = refs[11:]
    heads, rows, _ = t_ref.shape
    steps = own_buf.shape[0] // heads
    at = pl.program_id(0)
    place = pick_ref[0]
    slot = pick_ref[1]

    def own_copy(s):
        return pltpu.make_async_copy(
            cache_ref.at[0, slot, pl.ds(first_head + s * heads, heads)],
            own_buf.at[pl.ds(s * heads, heads)],
            sem_own.at[s],
        )

    def got_copy(s, j):
        return pltpu.make_async_copy(
            got_refs[j].at[pl.ds(s * heads, heads)],
            got_buf.at[pl.ds(s * heads, heads)],
            sem_got.at[s],
        )

    @pl.when(at == 0)
    def _():
        for s in range(steps):
            own_copy(s).start()
            for j in range(peers):

                @pl.when(place == j + 1)
                def _(s=s, j=j):
                    got_copy(s, j).start()

        if experts:
            line = iota((LANES, rows), 0)
            named = jnp.zeros((LANES, rows), F32)
            for k in range(ids_ref.shape[0]):
                hit = line % experts == ids_ref[k : k + 1, :]
                named = jnp.where(hit, weight_ref[k : k + 1, :], named)
            coarse = named.astype(BF).astype(F32)
            both = jnp.where(line < experts, coarse, named - coarse)
            both = jnp.where(line < 2 * experts, both, 0.0)
            out_ref[:, out_ref.shape[1] - LANES :] = jnp.transpose(both).astype(BF)

    own_copy(at).wait()

    @pl.when(place > 0)
    def _():
        got_copy(at, 0).wait()

    here = place == 0
    for i in range(heads):
        span = slice(i * 128, (i + 1) * 128)
        head = at * heads + i
        state = jnp.where(here, own_buf[head], got_buf[head].astype(F32))
        beta = lbt_ref[0][:, HEADS_A_STEP + i : HEADS_A_STEP + i + 1]
        read = mm(kq_ref[i], state.astype(BF))
        rest = beta * v_ref[:, span].astype(F32) - read[:rows]
        fixed = mm(t_ref[i], rest.astype(BF)).astype(BF)
        added = mm(mk_ref[i], fixed)
        o = read[rows:] + added[:rows]
        last = jnp.exp(jnp.sum(lb_ref[0][i : i + 1, :], axis=-1, keepdims=True))
        next_ref[i] = last * state + added[rows:]
        scaled = o / jnp.sqrt(jnp.mean(o * o, axis=-1, keepdims=True) + EPS) * gain_ref[...]
        gated = scaled * silu(gate_ref[:, span].astype(F32))
        mixed = (res_ref[:, span].astype(F32) + gated).astype(BF)
        out_ref[:, pl.ds(pl.multiple_of(head * 128, 128), 128)] = mixed


def resume(
    pick, cache, got, kq, t, mk, values, lb, lbt, gate, residual, gain, ids, weight, first, heads,
    experts,
):
    rows = values.shape[0]
    step = HEADS_A_STEP
    wide = heads * 128 + (LANES if experts else 0)
    base = first // step
    any_spec = pl.BlockSpec(memory_space=pl.ANY)
    cols = pl.BlockSpec((rows, step * 128), lambda i, p: (0, base + i))
    group = lambda i, p: (base + i, 0, 0)
    local_group = lambda i, p: (i, 0, 0)
    whole = lambda i, p: (0, 0)
    return pl.pallas_call(
        lambda *refs: resume_kernel(*refs, peers=len(got), first_head=first, experts=experts),
        grid_spec=pltpu.PrefetchScalarGridSpec(
            num_scalar_prefetch=1,
            grid=(heads // step,),
            in_specs=[any_spec]
            + [any_spec] * len(got)
            + [
                pl.BlockSpec((step,) + kq.shape[1:], local_group),
                pl.BlockSpec((step,) + t.shape[1:], local_group),
                pl.BlockSpec((step,) + mk.shape[1:], local_group),
                cols,
                pl.BlockSpec((1,) + lb.shape[1:], group),
                pl.BlockSpec((1,) + lbt.shape[1:], group),
                cols,
                cols,
                pl.BlockSpec((1, 128), whole),
                pl.BlockSpec(ids.shape, whole),
                pl.BlockSpec(weight.shape, whole),
            ],
            out_specs=[
                pl.BlockSpec((rows, wide), whole),
                pl.BlockSpec((step, 128, 128), lambda i, p: (i, 0, 0)),
            ],
            scratch_shapes=[
                pltpu.VMEM((heads, 128, 128), F32),
                pltpu.VMEM((heads, 128, 128), BF),
                pltpu.SemaphoreType.DMA((heads // step,)),
                pltpu.SemaphoreType.DMA((heads // step,)),
            ],
        ),
        out_shape=[
            jax.ShapeDtypeStruct((rows, wide), BF),
            jax.ShapeDtypeStruct((heads, 128, 128), F32),
        ],
        compiler_params=pltpu.CompilerParams(vmem_limit_bytes=VMEM_BYTES),
        cost_estimate=pl.CostEstimate(flops=1000, transcendentals=0, bytes_accessed=1000),
        name="resume",
    )(pick, cache, *got, kq, t, mk, values, lb, lbt, gate, residual, gain, ids, weight)


def expert_kernel(first_ref, *refs, blocks, parts, experts, all_experts, pieces):
    x_refs, refs = refs[: blocks * parts], refs[blocks * parts :]
    gain_ref, wg_ref, wu_ref, wd_ref, own_ref = refs[:5]
    other_refs, refs = refs[5 : 5 + pieces], refs[5 + pieces :]
    xs_ref, posr_ref, posc_ref, wr_ref, chosen_ref, slot_ref, rows_ref = refs
    step = pl.program_id(0)
    e = step
    rows = x_refs[0].shape[0]
    d = xs_ref.shape[1]
    pairs = blocks // 2
    two = 2 * rows

    @pl.when(step == 0)
    def _():
        gain = gain_ref[...]
        slab = 16
        a, b = iota((LANES, LANES), 0), iota((LANES, LANES), 1)
        first = first_ref[0]
        mine = ((a == first + b) | (a == first + b + all_experts)) & (b < experts)
        mine = mine.astype(F32).astype(BF)
        before = (iota((rows, rows), 0) > iota((rows, rows), 1)).astype(F32).astype(BF)
        for n in range(blocks):
            last = x_refs[n * parts + parts - 1]
            weight = mm(last[:, last.shape[1] - LANES :], mine)
            routed = weight > 0.0
            rank = mm(before, routed.astype(F32).astype(BF)) + float(n % 2 * MOST)
            rank = jnp.where(routed, rank, FAR)
            posc_ref[n] = rank
            posr_ref[n] = jnp.transpose(rank)
            wr_ref[n] = jnp.transpose(weight)

            def norm(s, carry, n=n):
                at = pl.multiple_of(s * slab, slab)
                pieces = [x_refs[n * parts + c][pl.ds(at, slab), :] for c in range(parts)]
                pieces[-1] = pieces[-1][:, : pieces[-1].shape[1] - LANES]
                x = jnp.concatenate(pieces, axis=1).astype(F32)
                mean = jnp.mean(x * x, axis=-1, keepdims=True)
                to = pl.multiple_of(n * rows + s * slab, slab)
                xs_ref[pl.ds(to, slab), :] = (x * (1.0 / jnp.sqrt(mean + EPS)) * gain).astype(BF)
                return carry

            lax.fori_loop(0, rows // slab, norm, 0, unroll=2)

    if True:
        for p in range(pairs):
            pos = [posr_ref[2 * p + c, pl.ds(e, 1), :] for c in range(2)]
            weight = [wr_ref[2 * p + c, pl.ds(e, 1), :] for c in range(2)]
            sel = iota((PAIR, two), 0).astype(F32) == jnp.concatenate(pos, axis=1)
            span = slice(p * PAIR, (p + 1) * PAIR)
            slot_ref[span, :] = jnp.broadcast_to(
                jnp.sum(
                    jnp.where(sel, jnp.concatenate(weight, axis=1), 0.0), axis=1, keepdims=True
                ),
                (PAIR, LANES),
            )
            chosen_ref[span, :] = mm(
                sel.astype(F32).astype(BF), xs_ref[p * two : (p + 1) * two, :]
            ).astype(BF)

    x = chosen_ref[...]
    hidden = silu(mm(x, wg_ref[e])) * mm(x, wu_ref[e]) * slot_ref[:, 0:1]
    done = mm(hidden.astype(BF), wd_ref[e]).astype(BF)
    to = pl.multiple_of(e * PAIR, 16)
    for p in range(pairs):
        rows_ref[p, pl.ds(to, PAIR), :] = done[p * PAIR : (p + 1) * PAIR]

    @pl.when(step == pl.num_programs(0) - 1)
    def _():
        lane = iota((two, experts * PAIR), 1).astype(F32)
        for p in range(pairs):
            at = jnp.concatenate([posc_ref[2 * p], posc_ref[2 * p + 1]], axis=0)
            hit = lane == at[:, 0:1]
            for n in range(1, experts):
                hit = hit | (lane == at[:, n : n + 1] + float(n * PAIR))
            both = mm(hit.astype(F32).astype(BF), rows_ref[p]).astype(BF)
            own_ref[p] = both[:rows]
            for n in range(pieces):
                other_refs[n][p] = both[rows:, n * d // pieces : (n + 1) * d // pieces]


def expert_stage(first, xs, parts, gain, w_gate, w_up, w_down, all_experts, pieces):
    experts, d, ff = w_gate.shape
    rows = xs[0].shape[0]
    blocks = len(xs) // parts
    pairs = blocks // 2
    one = pl.Buffered(1)
    outs = [jax.ShapeDtypeStruct((pairs, rows, d), BF)]
    outs += [jax.ShapeDtypeStruct((pairs, rows, d // pieces), BF)] * pieces
    whole3 = lambda s, m: (0, 0, 0)
    return pl.pallas_call(
        lambda *refs: expert_kernel(
            *refs, blocks=blocks, parts=parts, experts=experts, all_experts=all_experts,
            pieces=pieces,
        ),
        grid_spec=pltpu.PrefetchScalarGridSpec(
            num_scalar_prefetch=1,
            grid=(experts,),
            in_specs=[pl.BlockSpec(x.shape, lambda s, m: (0, 0), pipeline_mode=one) for x in xs]
            + [
                pl.BlockSpec((1, d), lambda s, m: (0, 0)),
                pl.BlockSpec(memory_space=pltpu.VMEM),
                pl.BlockSpec(memory_space=pltpu.VMEM),
                pl.BlockSpec(memory_space=pltpu.VMEM),
            ],
            out_specs=[pl.BlockSpec(out.shape, whole3) for out in outs],
            scratch_shapes=[
                pltpu.VMEM((blocks * rows, d), BF),
                pltpu.VMEM((blocks, LANES, rows), F32),
                pltpu.VMEM((blocks, rows, LANES), F32),
                pltpu.VMEM((blocks, LANES, rows), F32),
                pltpu.VMEM((pairs * PAIR, d), BF),
                pltpu.VMEM((pairs * PAIR, LANES), F32),
                pltpu.VMEM((pairs, experts * PAIR, d), BF),
            ],
        ),
        out_shape=outs,
        compiler_params=pltpu.CompilerParams(vmem_limit_bytes=VMEM_BYTES),
        cost_estimate=pl.CostEstimate(flops=1000, transcendentals=0, bytes_accessed=1000),
        name="experts",
    )(first, *xs, gain, w_gate, w_up, w_down)


def after(*xs):
    return lax.optimization_barrier(xs)


def swap(x, axis, bits, what):
    size = lax.axis_size(axis)
    with jax.named_scope(what):
        return lax.ppermute(x, axis, [(i, i ^ bits) for i in range(size)])


def local(
    residual_in,
    queries,
    keys_in,
    values_in,
    out_gate,
    log_decay,
    beta_rate,
    head_gain,
    moe_gain,
    state_cache,
    hit_holder,
    hit_slot,
    expert_ids,
    gate_weight,
    w_gate,
    w_up,
    w_down,
):
    rows, d = queries.shape
    head_count = log_decay.shape[0]
    holders = lax.axis_size("dp")
    group = lax.axis_size("expert")
    own_dp = lax.axis_index("dp")
    own_ep = lax.axis_index("expert")
    experts = w_gate.shape[0]
    pairs = group // 2
    all_experts = group * experts
    chunks = HEAD_CHUNKS
    starts = [sum(chunks[:g]) for g in range(len(chunks))]

    groups = head_count // HEADS_A_STEP
    lb = jnp.concatenate(
        [
            log_decay.reshape(groups, HEADS_A_STEP, rows),
            beta_rate.reshape(groups, HEADS_A_STEP, rows),
        ],
        axis=1,
    )
    lbt = lb.transpose(0, 2, 1)
    pick = jnp.stack([hit_holder[0] ^ own_dp, hit_slot[0]])

    wish = jnp.concatenate([hit_holder, hit_slot])
    asked = [swap(wish, "dp", j, f"hits{j}") for j in range(1, holders)]
    asked[0], lb, lbt, pick = after(asked[0], lb, lbt, pick)
    got = []
    for first, heads in zip(starts, chunks):
        pieces = pack(own_dp[None], asked, state_cache, first, heads)
        asked[0], *pieces = after(asked[0], *pieces)
        got.append(
            [swap(p, "dp", j + 1, f"state{first}from{j + 1}") for j, p in enumerate(pieces)]
        )

    lb = after(lb, asked[0])[0]
    mixed, states = [], []
    for g, (first, heads) in enumerate(zip(starts, chunks)):
        last = g == len(chunks) - 1
        kq, t, mk = prepare(queries, keys_in, lb, lbt, first, heads)
        m, s = resume(
            pick, state_cache, got[g], kq, t, mk, values_in, lb, lbt, out_gate, residual_in,
            head_gain[None], expert_ids.T, gate_weight.T, first, heads, all_experts if last else 0,
        )
        pick, lb = after(pick, lb, m)[:2]
        mixed.append(m)
        states.append(s)
    parts = len(chunks)
    next_state = jnp.concatenate(states, axis=0)[None]
    mixer_out = jnp.concatenate(mixed[:-1] + [mixed[-1][:, :-LANES]], axis=1)

    gain = moe_gain[None]
    first_expert = (own_ep * experts)[None].astype(jnp.int32)
    weights = (w_gate, w_up, w_down)
    if group == 8:
        whole = jnp.concatenate(mixed, axis=1)
        near = [mixed, [], [], []]
        for c in range(parts):
            near[2].append(swap(mixed[c], "expert", 4, f"rows{c}chip2"))
        near[3].append(swap(whole, "expert", 6, "rowschip3"))
        for c in range(parts):
            x = after(mixed[c], mixed[-1])[0]
            near[1].append(swap(x, "expert", 2, f"rows{c}chip1"))
        sums, ready = [], []
        gain, mixer_out, next_state = after(gain, mixer_out, next_state)
        for stage, pieces in zip(STAGES, PIECES):
            if stage == STAGES[-1]:
                gain = after(gain, *ready)[0]
            xs = []
            for r in stage:
                held = [after(x, own)[0] for x in near[r]] if r else near[r]
                xs += near[r]
                xs += [swap(x, "expert", 1, f"rows{c}pair{r}") for c, x in enumerate(held)]
            count = len(xs) // (2 * len(stage))
            own, *other = expert_stage(
                first_expert, xs, count, gain, *weights, all_experts, pieces
            )
            gain = after(gain, own)[0]
            came = [swap(o, "expert", 1, f"sums{stage[0]}pair") for o in other]
            wide = d // pieces
            for i, r in enumerate(stage):
                chip = [
                    own[i][:, n * wide : (n + 1) * wide].astype(F32) + came[n][i].astype(F32)
                    for n in range(pieces)
                ]
                if r in (1, 2):
                    chip = jnp.concatenate(chip, axis=1).astype(BF)
                    ready.append(chip)
                    chip = [swap(chip, "expert", 2 * r, f"sums{r}chip").astype(F32)]
                elif r == 3:
                    chip = [
                        swap(c.astype(BF), "expert", 2 * r, f"sums{r}chip").astype(F32)
                        for c in chip
                    ]
                sums.append(jnp.concatenate(chip, axis=1))
        expert_out = sum(sums).astype(BF)
    else:
        order = jnp.arange(group, dtype=jnp.int32) ^ own_ep
        x = lax.all_gather(jnp.concatenate(mixed, axis=1), "expert", axis=0)[order]
        sums = []
        for p in range(0, group, 8):
            xs = [x[p + i] for i in range(8)]
            own, *other = expert_stage(first_expert, xs, 1, gain, *weights, all_experts, 1)
            other = jnp.concatenate(other, axis=2)
            sums.append(jnp.stack([own, other], axis=1).reshape(8, rows, d))
        part = jnp.concatenate(sums, axis=0)[order]
        expert_out = lax.psum_scatter(part, "expert", scatter_dimension=0)
    return (mixer_out, expert_out, next_state)


def solution(mesh):
    both = ("dp", "expert")
    rows = P(both, None)
    placed = (
        rows,
        rows,
        rows,
        rows,
        rows,
        P(None, both),
        P(None, both),
        P(),
        P(),
        P(both, None, None, None, None),
        P(both),
        P(both),
        rows,
        rows,
        P("expert", None, None),
        P("expert", None, None),
        P("expert", None, None),
    )
    return jax.shard_map(
        local,
        mesh=mesh,
        in_specs=placed,
        out_specs=(rows, rows, P(both, None, None, None)),
        check_vma=False,
    )
```

```python
import jax
import jax.numpy as jnp
from jax import lax
from jax.experimental import pallas as pl
from jax.experimental.pallas import tpu as pltpu
from jax.sharding import PartitionSpec as P

MOST = 56
PAIR = 2 * MOST
EPS = 1e-06
HEADS_A_STEP = 4
HEAD_CHUNKS = (8, 8)
STAGES = ((0,), (1, 2), (3,))
PIECES = (1, 2, 4)
LANES = 128
FAR = -100000.0
BF = jnp.bfloat16
F32 = jnp.float32
MIB = 1024 * 1024


def iota(shape, dim):
    return lax.broadcasted_iota(jnp.int32, shape, dim)


def mm(a, b):
    return jnp.dot(a, b, preferred_element_type=F32)


def silu(x):
    return x / (1.0 + jnp.exp(-x))


def prepare_kernel(*refs, carried):
    q_ref, k_ref, lb_ref, lbt_ref = refs[:4]
    from_refs, refs = refs[4 : 4 + carried], refs[4 + carried :]
    kq_ref, t_ref, mk_ref = refs[:3]
    to_refs, sems = refs[3 : 3 + carried], refs[3 + carried]
    copies = [pltpu.make_async_copy(a, b, sems.at[n]) for n, (a, b) in enumerate(zip(from_refs, to_refs))]

    @pl.when(pl.program_id(0) == 0)
    def _():
        for copy in copies:
            copy.start()

    rows = q_ref.shape[0]
    dk = 128
    at_row = iota((rows, rows), 0)
    at_col = iota((rows, rows), 1)
    strict = at_row > at_col
    inclusive = at_row >= at_col
    lower = inclusive.astype(F32)
    upper = (at_row <= at_col).astype(F32)
    top = lax.Precision.HIGHEST
    total_row = jnp.dot(lb_ref[0], upper, precision=top, preferred_element_type=F32)
    total_col = jnp.dot(lower, lbt_ref[0], precision=top, preferred_element_type=F32)
    solved = []
    mixes = []
    for i in range(HEADS_A_STEP):
        span = slice(i * dk, (i + 1) * dk)
        q = q_ref[:, span].astype(F32)
        k = k_ref[:, span].astype(F32)
        q = q / jnp.sqrt(jnp.sum(q * q, axis=-1, keepdims=True) + EPS)
        k = k / jnp.sqrt(jnp.sum(k * k, axis=-1, keepdims=True) + EPS)
        l_col = total_col[:, i : i + 1]
        l_row = total_row[i : i + 1, :]
        beta = lbt_ref[0][:, HEADS_A_STEP + i : HEADS_A_STEP + i + 1]
        ratio = jnp.where(inclusive, jnp.exp(jnp.where(inclusive, l_col - l_row, 0.0)), 0.0)
        kb = k.astype(BF)
        both = lax.dot_general(
            jnp.concatenate([kb, q.astype(BF)], axis=0),
            kb,
            (((1,), (1,)), ((), ())),
            preferred_element_type=F32,
        )
        mix = jnp.where(strict, beta * ratio * both[:rows], 0.0)
        growth = jnp.exp(l_col)
        trail = jnp.exp(l_col[rows - 1 : rows, :] - l_col)
        kq_ref[i] = jnp.concatenate([k * (beta * growth), q * growth], axis=0).astype(BF)
        mk_ref[i] = jnp.concatenate(
            [ratio * both[rows:], jnp.transpose(k * trail)], axis=0
        ).astype(BF)
        mixes.append(mix)
        first = (at_row // 2 == at_col // 2) & strict
        solved.append((at_row == at_col).astype(F32) - jnp.where(first, mix, 0.0))
    size = 2
    while size < rows:
        here = (
            (at_row // (2 * size) == at_col // (2 * size))
            & ((at_row // size) % 2 == 1)
            & ((at_col // size) % 2 == 0)
        )
        for i in range(HEADS_A_STEP):
            t = solved[i].astype(BF)
            block = jnp.where(here, mixes[i], 0.0).astype(BF)
            solved[i] = solved[i] - mm(t, mm(block, t).astype(BF))
        size *= 2
    for i in range(HEADS_A_STEP):
        t_ref[i] = solved[i].astype(BF)

    @pl.when(pl.program_id(0) == pl.num_programs(0) - 1)
    def _():
        for copy in copies:
            copy.wait()


def prepare(queries, keys_in, lb, lbt, first, heads, carry):
    rows = queries.shape[0]
    groups = heads // HEADS_A_STEP
    base = first // HEADS_A_STEP
    wide = HEADS_A_STEP * 128
    carry = [pltpu.with_memory_space_constraint(w, pltpu.HBM) for w in carry]
    kq, t, mk, *carried = pl.pallas_call(
        lambda *refs: prepare_kernel(*refs, carried=len(carry)),
        grid=(groups,),
        in_specs=[
            pl.BlockSpec((rows, wide), lambda i: (0, base + i)),
            pl.BlockSpec((rows, wide), lambda i: (0, base + i)),
            pl.BlockSpec((1,) + lb.shape[1:], lambda i: (base + i, 0, 0)),
            pl.BlockSpec((1,) + lbt.shape[1:], lambda i: (base + i, 0, 0)),
        ]
        + [pl.BlockSpec(memory_space=pl.ANY)] * len(carry),
        out_specs=[
            pl.BlockSpec((HEADS_A_STEP, 2 * rows, 128), lambda i: (i, 0, 0)),
            pl.BlockSpec((HEADS_A_STEP, rows, rows), lambda i: (i, 0, 0)),
            pl.BlockSpec((HEADS_A_STEP, rows + 128, rows), lambda i: (i, 0, 0)),
        ]
        + [pl.BlockSpec(memory_space=pltpu.VMEM)] * len(carry),
        out_shape=[
            jax.ShapeDtypeStruct((heads, 2 * rows, 128), BF),
            jax.ShapeDtypeStruct((heads, rows, rows), BF),
            jax.ShapeDtypeStruct((heads, rows + 128, rows), BF),
        ]
        + [pltpu.VMEM(w.shape, w.dtype) for w in carry],
        scratch_shapes=[pltpu.SemaphoreType.DMA((max(1, len(carry)),))],
        compiler_params=pltpu.CompilerParams(vmem_limit_bytes=12 * MIB),
        cost_estimate=pl.CostEstimate(flops=1000, transcendentals=0, bytes_accessed=1000),
        name="prepare",
    )(queries, keys_in, lb, lbt, *carry)
    return kq, t, mk, carried


def pack_kernel(own_ref, *refs, peers, first):
    asked, cache_ref, outs = refs[:peers], refs[peers], refs[peers + 1 : 2 * peers + 1]
    buf, sems = refs[2 * peers + 1 :]
    heads = buf.shape[1]
    copies = []
    for j in range(peers):
        slot = jnp.where(asked[j][0] == own_ref[0], asked[j][1], 0)
        copies.append(
            pltpu.make_async_copy(
                cache_ref.at[0, slot, pl.ds(first, heads)], buf.at[j], sems.at[j]
            )
        )
        copies[-1].start()
    for j in range(peers):
        copies[j].wait()
        outs[j][...] = buf[j].astype(BF)


def pack(own, asked, cache, first, heads):
    peers = len(asked)
    shape = (heads,) + cache.shape[3:]
    return pl.pallas_call(
        lambda *refs: pack_kernel(*refs, peers=peers, first=first),
        grid_spec=pltpu.PrefetchScalarGridSpec(
            num_scalar_prefetch=1 + peers,
            grid=(1,),
            in_specs=[pl.BlockSpec(memory_space=pl.ANY)],
            out_specs=[pl.BlockSpec(shape, lambda i, *p: (0, 0, 0))] * peers,
            scratch_shapes=[
                pltpu.VMEM((peers,) + shape, F32),
                pltpu.SemaphoreType.DMA((peers,)),
            ],
        ),
        out_shape=[jax.ShapeDtypeStruct(shape, BF)] * peers,
        compiler_params=pltpu.CompilerParams(vmem_limit_bytes=12 * MIB),
        cost_estimate=pl.CostEstimate(flops=1000, transcendentals=0, bytes_accessed=1000),
        name="pack",
    )(own, *asked, cache)


def resume_kernel(pick_ref, *refs, peers, first_head, experts, carried):
    cache_ref, got_refs, refs = refs[0], refs[1 : 1 + peers], refs[1 + peers :]
    kq_ref, t_ref, mk_ref, v_ref, lb_ref, lbt_ref, gate_ref, res_ref, gain_ref = refs[:9]
    ids_ref, weight_ref = refs[9:11]
    from_refs, refs = refs[11 : 11 + carried], refs[11 + carried :]
    out_ref, next_ref = refs[:2]
    to_refs, refs = refs[2 : 2 + carried], refs[2 + carried :]
    own_buf, got_buf, sem_own, sem_got, sem_carry = refs
    copies = [
        pltpu.make_async_copy(a, b, sem_carry.at[n])
        for n, (a, b) in enumerate(zip(from_refs, to_refs))
    ]
    heads, rows, _ = t_ref.shape
    steps = own_buf.shape[0] // heads
    at = pl.program_id(0)
    place = pick_ref[0]
    slot = pick_ref[1]

    def own_copy(s):
        return pltpu.make_async_copy(
            cache_ref.at[0, slot, pl.ds(first_head + s * heads, heads)],
            own_buf.at[pl.ds(s * heads, heads)],
            sem_own.at[s],
        )

    def got_copy(s, j):
        return pltpu.make_async_copy(
            got_refs[j].at[pl.ds(s * heads, heads)],
            got_buf.at[pl.ds(s * heads, heads)],
            sem_got.at[s],
        )

    @pl.when(at == 0)
    def _():
        for s in range(steps):
            own_copy(s).start()
            for j in range(peers):

                @pl.when(place == j + 1)
                def _(s=s, j=j):
                    got_copy(s, j).start()

        for copy in copies:
            copy.start()
        if experts:
            line = iota((LANES, rows), 0)
            named = jnp.zeros((LANES, rows), F32)
            for k in range(ids_ref.shape[0]):
                hit = line % experts == ids_ref[k : k + 1, :]
                named = jnp.where(hit, weight_ref[k : k + 1, :], named)
            coarse = named.astype(BF).astype(F32)
            both = jnp.where(line < experts, coarse, named - coarse)
            both = jnp.where(line < 2 * experts, both, 0.0)
            out_ref[:, out_ref.shape[1] - LANES :] = jnp.transpose(both).astype(BF)

    own_copy(at).wait()

    @pl.when(place > 0)
    def _():
        got_copy(at, 0).wait()

    here = place == 0
    for i in range(heads):
        span = slice(i * 128, (i + 1) * 128)
        head = at * heads + i
        state = jnp.where(here, own_buf[head], got_buf[head].astype(F32))
        beta = lbt_ref[0][:, HEADS_A_STEP + i : HEADS_A_STEP + i + 1]
        read = mm(kq_ref[i], state.astype(BF))
        rest = beta * v_ref[:, span].astype(F32) - read[:rows]
        fixed = mm(t_ref[i], rest.astype(BF)).astype(BF)
        added = mm(mk_ref[i], fixed)
        o = read[rows:] + added[:rows]
        last = jnp.exp(jnp.sum(lb_ref[0][i : i + 1, :], axis=-1, keepdims=True))
        next_ref[i] = last * state + added[rows:]
        scaled = o / jnp.sqrt(jnp.mean(o * o, axis=-1, keepdims=True) + EPS) * gain_ref[...]
        gated = scaled * silu(gate_ref[:, span].astype(F32))
        mixed = (res_ref[:, span].astype(F32) + gated).astype(BF)
        out_ref[:, pl.ds(pl.multiple_of(head * 128, 128), 128)] = mixed

    @pl.when(at == steps - 1)
    def _():
        for copy in copies:
            copy.wait()


def resume(
    pick, cache, got, kq, t, mk, values, lb, lbt, gate, residual, gain, ids, weight, first, heads,
    experts, carry,
):
    rows = values.shape[0]
    step = HEADS_A_STEP
    carry = [pltpu.with_memory_space_constraint(w, pltpu.HBM) for w in carry]
    wide = heads * 128 + (LANES if experts else 0)
    base = first // step
    any_spec = pl.BlockSpec(memory_space=pl.ANY)
    cols = pl.BlockSpec((rows, step * 128), lambda i, p: (0, base + i))
    group = lambda i, p: (base + i, 0, 0)
    local_group = lambda i, p: (i, 0, 0)
    whole = lambda i, p: (0, 0)
    out, state, *carried = pl.pallas_call(
        lambda *refs: resume_kernel(
            *refs, peers=len(got), first_head=first, experts=experts, carried=len(carry)
        ),
        grid_spec=pltpu.PrefetchScalarGridSpec(
            num_scalar_prefetch=1,
            grid=(heads // step,),
            in_specs=[any_spec]
            + [any_spec] * len(got)
            + [
                pl.BlockSpec((step,) + kq.shape[1:], local_group),
                pl.BlockSpec((step,) + t.shape[1:], local_group),
                pl.BlockSpec((step,) + mk.shape[1:], local_group),
                cols,
                pl.BlockSpec((1,) + lb.shape[1:], group),
                pl.BlockSpec((1,) + lbt.shape[1:], group),
                cols,
                cols,
                pl.BlockSpec((1, 128), whole),
                pl.BlockSpec(ids.shape, whole),
                pl.BlockSpec(weight.shape, whole),
            ]
            + [any_spec] * len(carry),
            out_specs=[
                pl.BlockSpec((rows, wide), whole),
                pl.BlockSpec((step, 128, 128), lambda i, p: (i, 0, 0)),
            ]
            + [pl.BlockSpec(memory_space=pltpu.VMEM)] * len(carry),
            scratch_shapes=[
                pltpu.VMEM((heads, 128, 128), F32),
                pltpu.VMEM((heads, 128, 128), BF),
                pltpu.SemaphoreType.DMA((heads // step,)),
                pltpu.SemaphoreType.DMA((heads // step,)),
                pltpu.SemaphoreType.DMA((max(1, len(carry)),)),
            ],
        ),
        out_shape=[
            jax.ShapeDtypeStruct((rows, wide), BF),
            jax.ShapeDtypeStruct((heads, 128, 128), F32),
        ]
        + [pltpu.VMEM(w.shape, w.dtype) for w in carry],
        compiler_params=pltpu.CompilerParams(vmem_limit_bytes=12 * MIB),
        cost_estimate=pl.CostEstimate(flops=1000, transcendentals=0, bytes_accessed=1000),
        name="resume",
    )(pick, cache, *got, kq, t, mk, values, lb, lbt, gate, residual, gain, ids, weight, *carry)
    return out, state, carried


def expert_kernel(first_ref, *refs, blocks, parts, experts, all_experts, pieces):
    x_refs, refs = refs[: blocks * parts], refs[blocks * parts :]
    gain_ref, wg_ref, wu_ref, wd_ref, own_ref = refs[:5]
    other_refs, refs = refs[5 : 5 + pieces], refs[5 + pieces :]
    xs_ref, posr_ref, posc_ref, wr_ref, chosen_ref, slot_ref, rows_ref = refs
    step = pl.program_id(0)
    e = step
    rows = x_refs[0].shape[0]
    d = xs_ref.shape[1]
    pairs = blocks // 2
    two = 2 * rows

    @pl.when(step == 0)
    def _():
        gain = gain_ref[...]
        slab = 16
        a, b = iota((LANES, LANES), 0), iota((LANES, LANES), 1)
        first = first_ref[0]
        mine = ((a == first + b) | (a == first + b + all_experts)) & (b < experts)
        mine = mine.astype(F32).astype(BF)
        before = (iota((rows, rows), 0) > iota((rows, rows), 1)).astype(F32).astype(BF)
        for n in range(blocks):
            last = x_refs[n * parts + parts - 1]
            weight = mm(last[:, last.shape[1] - LANES :], mine)
            routed = weight > 0.0
            rank = mm(before, routed.astype(F32).astype(BF)) + float(n % 2 * MOST)
            rank = jnp.where(routed, rank, FAR)
            posc_ref[n] = rank
            posr_ref[n] = jnp.transpose(rank)
            wr_ref[n] = jnp.transpose(weight)

            def norm(s, carry, n=n):
                at = pl.multiple_of(s * slab, slab)
                pieces = [x_refs[n * parts + c][pl.ds(at, slab), :] for c in range(parts)]
                pieces[-1] = pieces[-1][:, : pieces[-1].shape[1] - LANES]
                x = jnp.concatenate(pieces, axis=1).astype(F32)
                mean = jnp.mean(x * x, axis=-1, keepdims=True)
                to = pl.multiple_of(n * rows + s * slab, slab)
                xs_ref[pl.ds(to, slab), :] = (x * (1.0 / jnp.sqrt(mean + EPS)) * gain).astype(BF)
                return carry

            lax.fori_loop(0, rows // slab, norm, 0, unroll=2)

    if True:
        for p in range(pairs):
            pos = [posr_ref[2 * p + c, pl.ds(e, 1), :] for c in range(2)]
            weight = [wr_ref[2 * p + c, pl.ds(e, 1), :] for c in range(2)]
            sel = iota((PAIR, two), 0).astype(F32) == jnp.concatenate(pos, axis=1)
            span = slice(p * PAIR, (p + 1) * PAIR)
            slot_ref[span, :] = jnp.broadcast_to(
                jnp.sum(
                    jnp.where(sel, jnp.concatenate(weight, axis=1), 0.0), axis=1, keepdims=True
                ),
                (PAIR, LANES),
            )
            chosen_ref[span, :] = mm(
                sel.astype(F32).astype(BF), xs_ref[p * two : (p + 1) * two, :]
            ).astype(BF)

    x = chosen_ref[...]
    hidden = silu(mm(x, wg_ref[e])) * mm(x, wu_ref[e]) * slot_ref[:, 0:1]
    done = mm(hidden.astype(BF), wd_ref[e]).astype(BF)
    to = pl.multiple_of(e * PAIR, 16)
    for p in range(pairs):
        rows_ref[p, pl.ds(to, PAIR), :] = done[p * PAIR : (p + 1) * PAIR]

    @pl.when(step == pl.num_programs(0) - 1)
    def _():
        lane = iota((two, experts * PAIR), 1).astype(F32)
        for p in range(pairs):
            at = jnp.concatenate([posc_ref[2 * p], posc_ref[2 * p + 1]], axis=0)
            hit = lane == at[:, 0:1]
            for n in range(1, experts):
                hit = hit | (lane == at[:, n : n + 1] + float(n * PAIR))
            both = mm(hit.astype(F32).astype(BF), rows_ref[p]).astype(BF)
            own_ref[p] = both[:rows]
            for n in range(pieces):
                other_refs[n][p] = both[rows:, n * d // pieces : (n + 1) * d // pieces]


def expert_stage(first, xs, parts, gain, w_gate, w_up, w_down, all_experts, pieces):
    experts, d, ff = w_gate.shape
    rows = xs[0].shape[0]
    blocks = len(xs) // parts
    pairs = blocks // 2
    one = pl.Buffered(1)
    outs = [jax.ShapeDtypeStruct((pairs, rows, d), BF)]
    outs += [jax.ShapeDtypeStruct((pairs, rows, d // pieces), BF)] * pieces
    whole3 = lambda s, m: (0, 0, 0)
    return pl.pallas_call(
        lambda *refs: expert_kernel(
            *refs, blocks=blocks, parts=parts, experts=experts, all_experts=all_experts,
            pieces=pieces,
        ),
        grid_spec=pltpu.PrefetchScalarGridSpec(
            num_scalar_prefetch=1,
            grid=(experts,),
            in_specs=[pl.BlockSpec(x.shape, lambda s, m: (0, 0), pipeline_mode=one) for x in xs]
            + [
                pl.BlockSpec((1, d), lambda s, m: (0, 0)),
                pl.BlockSpec(memory_space=pltpu.VMEM),
                pl.BlockSpec(memory_space=pltpu.VMEM),
                pl.BlockSpec(memory_space=pltpu.VMEM),
            ],
            out_specs=[pl.BlockSpec(out.shape, whole3) for out in outs],
            scratch_shapes=[
                pltpu.VMEM((blocks * rows, d), BF),
                pltpu.VMEM((blocks, LANES, rows), F32),
                pltpu.VMEM((blocks, rows, LANES), F32),
                pltpu.VMEM((blocks, LANES, rows), F32),
                pltpu.VMEM((pairs * PAIR, d), BF),
                pltpu.VMEM((pairs * PAIR, LANES), F32),
                pltpu.VMEM((pairs, experts * PAIR, d), BF),
            ],
        ),
        out_shape=outs,
        compiler_params=pltpu.CompilerParams(vmem_limit_bytes=(4 + 5 * pairs) * MIB),
        cost_estimate=pl.CostEstimate(flops=1000, transcendentals=0, bytes_accessed=1000),
        name="experts",
    )(first, *xs, gain, w_gate, w_up, w_down)


def after(*xs):
    return lax.optimization_barrier(xs)


def swap(x, axis, bits, what):
    size = lax.axis_size(axis)
    with jax.named_scope(what):
        return lax.ppermute(x, axis, [(i, i ^ bits) for i in range(size)])


def local(
    residual_in,
    queries,
    keys_in,
    values_in,
    out_gate,
    log_decay,
    beta_rate,
    head_gain,
    moe_gain,
    state_cache,
    hit_holder,
    hit_slot,
    expert_ids,
    gate_weight,
    w_gate,
    w_up,
    w_down,
):
    rows, d = queries.shape
    head_count = log_decay.shape[0]
    queries, keys_in, values_in, out_gate, residual_in, state_cache = (
        pltpu.with_memory_space_constraint(x, pltpu.HBM)
        for x in (queries, keys_in, values_in, out_gate, residual_in, state_cache)
    )
    holders = lax.axis_size("dp")
    group = lax.axis_size("expert")
    own_dp = lax.axis_index("dp")
    own_ep = lax.axis_index("expert")
    experts = w_gate.shape[0]
    pairs = group // 2
    all_experts = group * experts
    chunks = HEAD_CHUNKS
    starts = [sum(chunks[:g]) for g in range(len(chunks))]

    groups = head_count // HEADS_A_STEP
    lb = jnp.concatenate(
        [
            log_decay.reshape(groups, HEADS_A_STEP, rows),
            beta_rate.reshape(groups, HEADS_A_STEP, rows),
        ],
        axis=1,
    )
    lbt = lb.transpose(0, 2, 1)
    pick = jnp.stack([hit_holder[0] ^ own_dp, hit_slot[0]])

    wish = jnp.concatenate([hit_holder, hit_slot])
    asked = [swap(wish, "dp", j, f"hits{j}") for j in range(1, holders)]
    *ready, held = prepare(queries, keys_in, lb, lbt, 0, chunks[0], ())
    asked[0], lb, lbt, pick, *ready = after(asked[0], lb, lbt, pick, *ready)
    got = []
    for first, heads in zip(starts, chunks):
        pieces = pack(own_dp[None], asked, state_cache, first, heads)
        asked[0], *pieces = after(asked[0], *pieces)
        got.append(
            [swap(p, "dp", j + 1, f"state{first}from{j + 1}") for j, p in enumerate(pieces)]
        )

    lb = after(lb, asked[0])[0]
    mixed, states = [], []
    for g, (first, heads) in enumerate(zip(starts, chunks)):
        last = g == len(chunks) - 1
        if g:
            more = (w_up, w_down) if g == 1 else ()
            *ready, new = prepare(queries, keys_in, lb, lbt, first, heads, more)
            held = held + new
        kq, t, mk = ready
        more = (w_gate,) if g == 1 else ()
        m, s, new = resume(
            pick, state_cache, got[g], kq, t, mk, values_in, lb, lbt, out_gate, residual_in,
            head_gain[None], expert_ids.T, gate_weight.T, first, heads, all_experts if last else 0,
            more,
        )
        held = new + held
        pick, lb = after(pick, lb, m)[:2]
        mixed.append(m)
        states.append(s)
    parts = len(chunks)
    next_state = jnp.concatenate(states, axis=0)[None]
    mixer_out = jnp.concatenate(mixed[:-1] + [mixed[-1][:, :-LANES]], axis=1)

    gain = moe_gain[None]
    first_expert = (own_ep * experts)[None].astype(jnp.int32)
    weights = held
    if group == 8:
        near = [mixed, [], [], []]
        for c in range(parts):
            near[2].append(swap(mixed[c], "expert", 4, f"rows{c}chip2"))
            near[3].append(swap(near[2][c], "expert", 2, f"rows{c}chip3"))
        for c in range(parts):
            x = after(mixed[c], mixed[-1])[0]
            near[1].append(swap(x, "expert", 2, f"rows{c}chip1"))
        sums, ready, landed = [], [], []
        gain, mixer_out, next_state = after(gain, mixer_out, next_state)
        for stage, pieces in zip(STAGES, PIECES):
            if stage == STAGES[0]:
                gain = after(gain, near[2][0])[0]
            if stage == STAGES[-1]:
                gain = after(gain, *ready)[0]
            xs = []
            for r in stage:
                held = [after(x, own)[0] for x in near[r]] if r else near[r]
                xs += near[r]
                xs += [swap(x, "expert", 1, f"rows{c}pair{r}") for c, x in enumerate(held)]
            count = len(xs) // (2 * len(stage))
            own, *other = expert_stage(
                first_expert, xs, count, gain, *weights, all_experts, pieces
            )
            gain = after(gain, own)[0]
            came = [swap(o, "expert", 1, f"sums{stage[0]}pair") for o in other]
            wide = d // pieces
            for i, r in enumerate(stage):
                chip = [
                    own[i][:, n * wide : (n + 1) * wide].astype(F32) + came[n][i].astype(F32)
                    for n in range(pieces)
                ]
                if r in (1, 2):
                    chip = jnp.concatenate(chip, axis=1).astype(BF)
                    ready.append(chip)
                    chip = swap(chip, "expert", 2 * r, f"sums{r}chip")
                    landed.append(chip)
                    chip = [chip.astype(F32)]
                elif r == 3:
                    chip = [c.astype(BF) for c in chip]
                    half = pieces // 2
                    chip[half:] = after(*chip[half:], *landed)[:half]
                    chip = [swap(c, "expert", 2 * r, f"sums{r}chip").astype(F32) for c in chip]
                sums.append(jnp.concatenate(chip, axis=1))
        expert_out = sum(sums).astype(BF)
    else:
        order = jnp.arange(group, dtype=jnp.int32) ^ own_ep
        x = lax.all_gather(jnp.concatenate(mixed, axis=1), "expert", axis=0)[order]
        sums = []
        for p in range(0, group, 8):
            xs = [x[p + i] for i in range(8)]
            own, *other = expert_stage(first_expert, xs, 1, gain, *weights, all_experts, 1)
            other = jnp.concatenate(other, axis=2)
            sums.append(jnp.stack([own, other], axis=1).reshape(8, rows, d))
        part = jnp.concatenate(sums, axis=0)[order]
        expert_out = lax.psum_scatter(part, "expert", scatter_dimension=0)
    return (mixer_out, expert_out, next_state)


def solution(mesh):
    both = ("dp", "expert")
    rows = P(both, None)
    placed = (
        rows,
        rows,
        rows,
        rows,
        rows,
        P(None, both),
        P(None, both),
        P(),
        P(),
        P(both, None, None, None, None),
        P(both),
        P(both),
        rows,
        rows,
        P("expert", None, None),
        P("expert", None, None),
        P("expert", None, None),
    )
    return jax.shard_map(
        local,
        mesh=mesh,
        in_specs=placed,
        out_specs=(rows, rows, P(both, None, None, None)),
        check_vma=False,
    )
```

```python
import jax
import jax.numpy as jnp
from jax import lax
from jax.experimental import pallas as pl
from jax.experimental.pallas import tpu as pltpu
from jax.sharding import PartitionSpec as P

MOST = 56
PAIR = 2 * MOST
EPS = 1e-06
HEADS_A_STEP = 4
HEAD_CHUNKS = (8, 8)
STAGES = ((0,), (1, 2), (3,))
PIECES = (1, 2, 4)
LANES = 128
FAR = -100000.0
BF = jnp.bfloat16
F32 = jnp.float32
MIB = 1024 * 1024


def iota(shape, dim):
    return lax.broadcasted_iota(jnp.int32, shape, dim)


def mm(a, b):
    return jnp.dot(a, b, preferred_element_type=F32)


def silu(x):
    return x / (1.0 + jnp.exp(-x))


def prepare_kernel(*refs, carried):
    q_ref, k_ref, lb_ref, lbt_ref = refs[:4]
    from_refs, refs = refs[4 : 4 + carried], refs[4 + carried :]
    kq_ref, t_ref, mk_ref = refs[:3]
    to_refs, sems = refs[3 : 3 + carried], refs[3 + carried]
    copies = [pltpu.make_async_copy(a, b, sems.at[n]) for n, (a, b) in enumerate(zip(from_refs, to_refs))]

    @pl.when(pl.program_id(0) == 0)
    def _():
        for copy in copies:
            copy.start()

    rows = q_ref.shape[0]
    dk = 128
    at_row = iota((rows, rows), 0)
    at_col = iota((rows, rows), 1)
    strict = at_row > at_col
    inclusive = at_row >= at_col
    lower = inclusive.astype(F32)
    upper = (at_row <= at_col).astype(F32)
    top = lax.Precision.HIGHEST
    total_row = jnp.dot(lb_ref[0], upper, precision=top, preferred_element_type=F32)
    total_col = jnp.dot(lower, lbt_ref[0], precision=top, preferred_element_type=F32)
    solved = []
    mixes = []
    for i in range(HEADS_A_STEP):
        span = slice(i * dk, (i + 1) * dk)
        q = q_ref[:, span].astype(F32)
        k = k_ref[:, span].astype(F32)
        q = q / jnp.sqrt(jnp.sum(q * q, axis=-1, keepdims=True) + EPS)
        k = k / jnp.sqrt(jnp.sum(k * k, axis=-1, keepdims=True) + EPS)
        l_col = total_col[:, i : i + 1]
        l_row = total_row[i : i + 1, :]
        beta = lbt_ref[0][:, HEADS_A_STEP + i : HEADS_A_STEP + i + 1]
        ratio = jnp.where(inclusive, jnp.exp(jnp.where(inclusive, l_col - l_row, 0.0)), 0.0)
        kb = k.astype(BF)
        both = lax.dot_general(
            jnp.concatenate([kb, q.astype(BF)], axis=0),
            kb,
            (((1,), (1,)), ((), ())),
            preferred_element_type=F32,
        )
        mix = jnp.where(strict, beta * ratio * both[:rows], 0.0)
        growth = jnp.exp(l_col)
        trail = jnp.exp(l_col[rows - 1 : rows, :] - l_col)
        kq_ref[i] = jnp.concatenate([k * (beta * growth), q * growth], axis=0).astype(BF)
        mk_ref[i] = jnp.concatenate(
            [ratio * both[rows:], jnp.transpose(k * trail)], axis=0
        ).astype(BF)
        mixes.append(mix)
        first = (at_row // 2 == at_col // 2) & strict
        solved.append((at_row == at_col).astype(F32) - jnp.where(first, mix, 0.0))
    size = 2
    while size < rows:
        here = (
            (at_row // (2 * size) == at_col // (2 * size))
            & ((at_row // size) % 2 == 1)
            & ((at_col // size) % 2 == 0)
        )
        for i in range(HEADS_A_STEP):
            t = solved[i].astype(BF)
            block = jnp.where(here, mixes[i], 0.0).astype(BF)
            solved[i] = solved[i] - mm(t, mm(block, t).astype(BF))
        size *= 2
    for i in range(HEADS_A_STEP):
        t_ref[i] = solved[i].astype(BF)

    @pl.when(pl.program_id(0) == pl.num_programs(0) - 1)
    def _():
        for copy in copies:
            copy.wait()


def prepare(queries, keys_in, lb, lbt, first, heads, carry):
    rows = queries.shape[0]
    groups = heads // HEADS_A_STEP
    base = first // HEADS_A_STEP
    wide = HEADS_A_STEP * 128
    carry = [pltpu.with_memory_space_constraint(w, pltpu.HBM) for w in carry]
    kq, t, mk, *carried = pl.pallas_call(
        lambda *refs: prepare_kernel(*refs, carried=len(carry)),
        grid=(groups,),
        in_specs=[
            pl.BlockSpec((rows, wide), lambda i: (0, base + i)),
            pl.BlockSpec((rows, wide), lambda i: (0, base + i)),
            pl.BlockSpec((1,) + lb.shape[1:], lambda i: (base + i, 0, 0)),
            pl.BlockSpec((1,) + lbt.shape[1:], lambda i: (base + i, 0, 0)),
        ]
        + [pl.BlockSpec(memory_space=pl.ANY)] * len(carry),
        out_specs=[
            pl.BlockSpec((HEADS_A_STEP, 2 * rows, 128), lambda i: (i, 0, 0)),
            pl.BlockSpec((HEADS_A_STEP, rows, rows), lambda i: (i, 0, 0)),
            pl.BlockSpec((HEADS_A_STEP, rows + 128, rows), lambda i: (i, 0, 0)),
        ]
        + [pl.BlockSpec(memory_space=pltpu.VMEM)] * len(carry),
        out_shape=[
            jax.ShapeDtypeStruct((heads, 2 * rows, 128), BF),
            jax.ShapeDtypeStruct((heads, rows, rows), BF),
            jax.ShapeDtypeStruct((heads, rows + 128, rows), BF),
        ]
        + [pltpu.VMEM(w.shape, w.dtype) for w in carry],
        scratch_shapes=[pltpu.SemaphoreType.DMA((max(1, len(carry)),))],
        compiler_params=pltpu.CompilerParams(vmem_limit_bytes=12 * MIB),
        cost_estimate=pl.CostEstimate(flops=1000, transcendentals=0, bytes_accessed=1000),
        name="prepare",
    )(queries, keys_in, lb, lbt, *carry)
    return kq, t, mk, carried


def pack_kernel(own_ref, *refs, peers, first):
    asked, cache_ref, outs = refs[:peers], refs[peers], refs[peers + 1 : 2 * peers + 1]
    buf, sems = refs[2 * peers + 1 :]
    heads = buf.shape[1]
    copies = []
    for j in range(peers):
        slot = jnp.where(asked[j][0] == own_ref[0], asked[j][1], 0)
        copies.append(
            pltpu.make_async_copy(
                cache_ref.at[0, slot, pl.ds(first, heads)], buf.at[j], sems.at[j]
            )
        )
        copies[-1].start()
    for j in range(peers):
        copies[j].wait()
        outs[j][...] = buf[j].astype(BF)


def pack(own, asked, cache, first, heads):
    peers = len(asked)
    shape = (heads,) + cache.shape[3:]
    return pl.pallas_call(
        lambda *refs: pack_kernel(*refs, peers=peers, first=first),
        grid_spec=pltpu.PrefetchScalarGridSpec(
            num_scalar_prefetch=1 + peers,
            grid=(1,),
            in_specs=[pl.BlockSpec(memory_space=pl.ANY)],
            out_specs=[pl.BlockSpec(shape, lambda i, *p: (0, 0, 0))] * peers,
            scratch_shapes=[
                pltpu.VMEM((peers,) + shape, F32),
                pltpu.SemaphoreType.DMA((peers,)),
            ],
        ),
        out_shape=[jax.ShapeDtypeStruct(shape, BF)] * peers,
        compiler_params=pltpu.CompilerParams(vmem_limit_bytes=12 * MIB),
        cost_estimate=pl.CostEstimate(flops=1000, transcendentals=0, bytes_accessed=1000),
        name="pack",
    )(own, *asked, cache)


def resume_kernel(pick_ref, *refs, peers, first_head, experts, carried):
    cache_ref, got_refs, refs = refs[0], refs[1 : 1 + peers], refs[1 + peers :]
    kq_ref, t_ref, mk_ref, v_ref, lb_ref, lbt_ref, gate_ref, res_ref, gain_ref = refs[:9]
    ids_ref, weight_ref = refs[9:11]
    from_refs, refs = refs[11 : 11 + carried], refs[11 + carried :]
    out_ref, next_ref = refs[:2]
    to_refs, refs = refs[2 : 2 + carried], refs[2 + carried :]
    own_buf, got_buf, sem_own, sem_got, sem_carry = refs
    copies = [
        pltpu.make_async_copy(a, b, sem_carry.at[n])
        for n, (a, b) in enumerate(zip(from_refs, to_refs))
    ]
    heads, rows, _ = t_ref.shape
    steps = own_buf.shape[0] // heads
    at = pl.program_id(0)
    place = pick_ref[0]
    slot = pick_ref[1]

    def own_copy(s):
        return pltpu.make_async_copy(
            cache_ref.at[0, slot, pl.ds(first_head + s * heads, heads)],
            own_buf.at[pl.ds(s * heads, heads)],
            sem_own.at[s],
        )

    def got_copy(s, j):
        return pltpu.make_async_copy(
            got_refs[j].at[pl.ds(s * heads, heads)],
            got_buf.at[pl.ds(s * heads, heads)],
            sem_got.at[s],
        )

    @pl.when(at == 0)
    def _():
        for s in range(steps):
            own_copy(s).start()
            for j in range(peers):

                @pl.when(place == j + 1)
                def _(s=s, j=j):
                    got_copy(s, j).start()

        for copy in copies:
            copy.start()
        if experts:
            line = iota((LANES, rows), 0)
            named = jnp.zeros((LANES, rows), F32)
            for k in range(ids_ref.shape[0]):
                hit = line % experts == ids_ref[k : k + 1, :]
                named = jnp.where(hit, weight_ref[k : k + 1, :], named)
            coarse = named.astype(BF).astype(F32)
            both = jnp.where(line < experts, coarse, named - coarse)
            both = jnp.where(line < 2 * experts, both, 0.0)
            out_ref[:, out_ref.shape[1] - LANES :] = jnp.transpose(both).astype(BF)

    own_copy(at).wait()

    @pl.when(place > 0)
    def _():
        got_copy(at, 0).wait()

    here = place == 0
    for i in range(heads):
        span = slice(i * 128, (i + 1) * 128)
        head = at * heads + i
        state = jnp.where(here, own_buf[head], got_buf[head].astype(F32))
        beta = lbt_ref[0][:, HEADS_A_STEP + i : HEADS_A_STEP + i + 1]
        read = mm(kq_ref[i], state.astype(BF))
        rest = beta * v_ref[:, span].astype(F32) - read[:rows]
        fixed = mm(t_ref[i], rest.astype(BF)).astype(BF)
        added = mm(mk_ref[i], fixed)
        o = read[rows:] + added[:rows]
        last = jnp.exp(jnp.sum(lb_ref[0][i : i + 1, :], axis=-1, keepdims=True))
        next_ref[i] = last * state + added[rows:]
        scaled = o / jnp.sqrt(jnp.mean(o * o, axis=-1, keepdims=True) + EPS) * gain_ref[...]
        gated = scaled * silu(gate_ref[:, span].astype(F32))
        mixed = (res_ref[:, span].astype(F32) + gated).astype(BF)
        out_ref[:, pl.ds(pl.multiple_of(head * 128, 128), 128)] = mixed

    @pl.when(at == steps - 1)
    def _():
        for copy in copies:
            copy.wait()


def resume(
    pick, cache, got, kq, t, mk, values, lb, lbt, gate, residual, gain, ids, weight, first, heads,
    experts, carry,
):
    rows = values.shape[0]
    step = HEADS_A_STEP
    carry = [pltpu.with_memory_space_constraint(w, pltpu.HBM) for w in carry]
    wide = heads * 128 + (LANES if experts else 0)
    base = first // step
    any_spec = pl.BlockSpec(memory_space=pl.ANY)
    cols = pl.BlockSpec((rows, step * 128), lambda i, p: (0, base + i))
    group = lambda i, p: (base + i, 0, 0)
    local_group = lambda i, p: (i, 0, 0)
    whole = lambda i, p: (0, 0)
    out, state, *carried = pl.pallas_call(
        lambda *refs: resume_kernel(
            *refs, peers=len(got), first_head=first, experts=experts, carried=len(carry)
        ),
        grid_spec=pltpu.PrefetchScalarGridSpec(
            num_scalar_prefetch=1,
            grid=(heads // step,),
            in_specs=[any_spec]
            + [any_spec] * len(got)
            + [
                pl.BlockSpec((step,) + kq.shape[1:], local_group),
                pl.BlockSpec((step,) + t.shape[1:], local_group),
                pl.BlockSpec((step,) + mk.shape[1:], local_group),
                cols,
                pl.BlockSpec((1,) + lb.shape[1:], group),
                pl.BlockSpec((1,) + lbt.shape[1:], group),
                cols,
                cols,
                pl.BlockSpec((1, 128), whole),
                pl.BlockSpec(ids.shape, whole),
                pl.BlockSpec(weight.shape, whole),
            ]
            + [any_spec] * len(carry),
            out_specs=[
                pl.BlockSpec((rows, wide), whole),
                pl.BlockSpec((step, 128, 128), lambda i, p: (i, 0, 0)),
            ]
            + [pl.BlockSpec(memory_space=pltpu.VMEM)] * len(carry),
            scratch_shapes=[
                pltpu.VMEM((heads, 128, 128), F32),
                pltpu.VMEM((heads, 128, 128), BF),
                pltpu.SemaphoreType.DMA((heads // step,)),
                pltpu.SemaphoreType.DMA((heads // step,)),
                pltpu.SemaphoreType.DMA((max(1, len(carry)),)),
            ],
        ),
        out_shape=[
            jax.ShapeDtypeStruct((rows, wide), BF),
            jax.ShapeDtypeStruct((heads, 128, 128), F32),
        ]
        + [pltpu.VMEM(w.shape, w.dtype) for w in carry],
        compiler_params=pltpu.CompilerParams(vmem_limit_bytes=12 * MIB),
        cost_estimate=pl.CostEstimate(flops=1000, transcendentals=0, bytes_accessed=1000),
        name="resume",
    )(pick, cache, *got, kq, t, mk, values, lb, lbt, gate, residual, gain, ids, weight, *carry)
    return out, state, carried


def expert_kernel(first_ref, *refs, blocks, parts, experts, all_experts, pieces):
    x_refs, refs = refs[: blocks * parts], refs[blocks * parts :]
    gain_ref, wg_ref, wu_ref, wd_ref, own_ref = refs[:5]
    other_refs, refs = refs[5 : 5 + pieces], refs[5 + pieces :]
    xs_ref, posr_ref, posc_ref, wr_ref, chosen_ref, slot_ref, rows_ref = refs
    step = pl.program_id(0)
    e = step
    rows = x_refs[0].shape[0]
    d = xs_ref.shape[1]
    pairs = blocks // 2
    two = 2 * rows

    @pl.when(step == 0)
    def _():
        gain = gain_ref[...]
        slab = 16
        a, b = iota((LANES, LANES), 0), iota((LANES, LANES), 1)
        first = first_ref[0]
        mine = ((a == first + b) | (a == first + b + all_experts)) & (b < experts)
        mine = mine.astype(F32).astype(BF)
        before = (iota((rows, rows), 0) > iota((rows, rows), 1)).astype(F32).astype(BF)
        for n in range(blocks):
            last = x_refs[n * parts + parts - 1]
            weight = mm(last[:, last.shape[1] - LANES :], mine)
            routed = weight > 0.0
            rank = mm(before, routed.astype(F32).astype(BF)) + float(n % 2 * MOST)
            rank = jnp.where(routed, rank, FAR)
            posc_ref[n] = rank
            posr_ref[n] = jnp.transpose(rank)
            wr_ref[n] = jnp.transpose(weight)

            def norm(s, carry, n=n):
                at = pl.multiple_of(s * slab, slab)
                pieces = [x_refs[n * parts + c][pl.ds(at, slab), :] for c in range(parts)]
                pieces[-1] = pieces[-1][:, : pieces[-1].shape[1] - LANES]
                x = jnp.concatenate(pieces, axis=1).astype(F32)
                mean = jnp.mean(x * x, axis=-1, keepdims=True)
                to = pl.multiple_of(n * rows + s * slab, slab)
                xs_ref[pl.ds(to, slab), :] = (x * (1.0 / jnp.sqrt(mean + EPS)) * gain).astype(BF)
                return carry

            lax.fori_loop(0, rows // slab, norm, 0, unroll=2)

    if True:
        for p in range(pairs):
            pos = [posr_ref[2 * p + c, pl.ds(e, 1), :] for c in range(2)]
            weight = [wr_ref[2 * p + c, pl.ds(e, 1), :] for c in range(2)]
            sel = iota((PAIR, two), 0).astype(F32) == jnp.concatenate(pos, axis=1)
            span = slice(p * PAIR, (p + 1) * PAIR)
            slot_ref[span, :] = jnp.broadcast_to(
                jnp.sum(
                    jnp.where(sel, jnp.concatenate(weight, axis=1), 0.0), axis=1, keepdims=True
                ),
                (PAIR, LANES),
            )
            chosen_ref[span, :] = mm(
                sel.astype(F32).astype(BF), xs_ref[p * two : (p + 1) * two, :]
            ).astype(BF)

    x = chosen_ref[...]
    hidden = silu(mm(x, wg_ref[e])) * mm(x, wu_ref[e]) * slot_ref[:, 0:1]
    done = mm(hidden.astype(BF), wd_ref[e]).astype(BF)
    to = pl.multiple_of(e * PAIR, 16)
    for p in range(pairs):
        rows_ref[p, pl.ds(to, PAIR), :] = done[p * PAIR : (p + 1) * PAIR]

    @pl.when(step == pl.num_programs(0) - 1)
    def _():
        lane = iota((two, experts * PAIR), 1).astype(F32)
        for p in range(pairs):
            at = jnp.concatenate([posc_ref[2 * p], posc_ref[2 * p + 1]], axis=0)
            hit = lane == at[:, 0:1]
            for n in range(1, experts):
                hit = hit | (lane == at[:, n : n + 1] + float(n * PAIR))
            both = mm(hit.astype(F32).astype(BF), rows_ref[p]).astype(BF)
            own_ref[p] = both[:rows]
            for n in range(pieces):
                other_refs[n][p] = both[rows:, n * d // pieces : (n + 1) * d // pieces]


def expert_stage(first, xs, parts, gain, w_gate, w_up, w_down, all_experts, pieces):
    experts, d, ff = w_gate.shape
    rows = xs[0].shape[0]
    blocks = len(xs) // parts
    pairs = blocks // 2
    one = pl.Buffered(1)
    outs = [jax.ShapeDtypeStruct((pairs, rows, d), BF)]
    outs += [jax.ShapeDtypeStruct((pairs, rows, d // pieces), BF)] * pieces
    whole3 = lambda s, m: (0, 0, 0)
    return pl.pallas_call(
        lambda *refs: expert_kernel(
            *refs, blocks=blocks, parts=parts, experts=experts, all_experts=all_experts,
            pieces=pieces,
        ),
        grid_spec=pltpu.PrefetchScalarGridSpec(
            num_scalar_prefetch=1,
            grid=(experts,),
            in_specs=[pl.BlockSpec(x.shape, lambda s, m: (0, 0), pipeline_mode=one) for x in xs]
            + [
                pl.BlockSpec((1, d), lambda s, m: (0, 0)),
                pl.BlockSpec(memory_space=pltpu.VMEM),
                pl.BlockSpec(memory_space=pltpu.VMEM),
                pl.BlockSpec(memory_space=pltpu.VMEM),
            ],
            out_specs=[pl.BlockSpec(out.shape, whole3) for out in outs],
            scratch_shapes=[
                pltpu.VMEM((blocks * rows, d), BF),
                pltpu.VMEM((blocks, LANES, rows), F32),
                pltpu.VMEM((blocks, rows, LANES), F32),
                pltpu.VMEM((blocks, LANES, rows), F32),
                pltpu.VMEM((pairs * PAIR, d), BF),
                pltpu.VMEM((pairs * PAIR, LANES), F32),
                pltpu.VMEM((pairs, experts * PAIR, d), BF),
            ],
        ),
        out_shape=outs,
        compiler_params=pltpu.CompilerParams(vmem_limit_bytes=(4 + 5 * pairs) * MIB),
        cost_estimate=pl.CostEstimate(flops=1000, transcendentals=0, bytes_accessed=1000),
        name="experts",
    )(first, *xs, gain, w_gate, w_up, w_down)


def after(*xs):
    return lax.optimization_barrier(xs)


def swap(x, axis, bits, what):
    size = lax.axis_size(axis)
    with jax.named_scope(what):
        return lax.ppermute(x, axis, [(i, i ^ bits) for i in range(size)])


def local(
    residual_in,
    queries,
    keys_in,
    values_in,
    out_gate,
    log_decay,
    beta_rate,
    head_gain,
    moe_gain,
    state_cache,
    hit_holder,
    hit_slot,
    expert_ids,
    gate_weight,
    w_gate,
    w_up,
    w_down,
):
    rows, d = queries.shape
    head_count = log_decay.shape[0]
    queries, keys_in, values_in, out_gate, residual_in, state_cache, ids_t, weight_t, head_gain = (
        pltpu.with_memory_space_constraint(x, pltpu.HBM)
        for x in (
            queries, keys_in, values_in, out_gate, residual_in, state_cache, expert_ids.T,
            gate_weight.T, head_gain[None],
        )
    )
    holders = lax.axis_size("dp")
    group = lax.axis_size("expert")
    own_dp = lax.axis_index("dp")
    own_ep = lax.axis_index("expert")
    experts = w_gate.shape[0]
    pairs = group // 2
    all_experts = group * experts
    chunks = HEAD_CHUNKS
    starts = [sum(chunks[:g]) for g in range(len(chunks))]

    groups = head_count // HEADS_A_STEP
    lb = jnp.concatenate(
        [
            log_decay.reshape(groups, HEADS_A_STEP, rows),
            beta_rate.reshape(groups, HEADS_A_STEP, rows),
        ],
        axis=1,
    )
    lbt = lb.transpose(0, 2, 1)
    pick = jnp.stack([hit_holder[0] ^ own_dp, hit_slot[0]])

    wish = jnp.concatenate([hit_holder, hit_slot])
    asked = [swap(wish, "dp", j, f"hits{j}") for j in range(1, holders)]
    asked[0], lb, lbt, pick = after(asked[0], lb, lbt, pick)
    got = []
    for first, heads in zip(starts, chunks):
        pieces = pack(own_dp[None], asked, state_cache, first, heads)
        asked[0], *pieces = after(asked[0], *pieces)
        got.append(
            [swap(p, "dp", j + 1, f"state{first}from{j + 1}") for j, p in enumerate(pieces)]
        )

    lb = after(lb, asked[0])[0]
    mixed, states, held = [], [], []
    carry = {("prepare", 1): (w_up, w_down), ("resume", 1): (w_gate,)}
    for g, (first, heads) in enumerate(zip(starts, chunks)):
        last = g == len(chunks) - 1
        *ready, new = prepare(queries, keys_in, lb, lbt, first, heads, carry.pop(("prepare", g), ()))
        held += new
        kq, t, mk = ready
        more = carry.pop(("resume", g), ())
        m, s, new = resume(
            pick, state_cache, got[g], kq, t, mk, values_in, lb, lbt, out_gate, residual_in,
            head_gain, ids_t, weight_t, first, heads, all_experts if last else 0,
            more,
        )
        held += new
        pick, lb = after(pick, lb, m)[:2]
        mixed.append(m)
        states.append(s)
    parts = len(chunks)
    next_state = jnp.concatenate(states, axis=0)[None]
    mixer_out = jnp.concatenate(mixed[:-1] + [mixed[-1][:, :-LANES]], axis=1)

    gain = moe_gain[None]
    first_expert = (own_ep * experts)[None].astype(jnp.int32)
    weights = [held[n] for n in (2, 0, 1)]
    if group == 8:
        near = [mixed, [], [], []]
        for c in range(parts):
            near[2].append(swap(mixed[c], "expert", 4, f"rows{c}chip2"))
            near[3].append(swap(near[2][c], "expert", 2, f"rows{c}chip3"))
        for c in range(parts):
            x = after(mixed[c], mixed[-1])[0]
            near[1].append(swap(x, "expert", 2, f"rows{c}chip1"))
        sums, ready, landed = [], [], []
        gain, mixer_out, next_state = after(gain, mixer_out, next_state)
        for stage, pieces in zip(STAGES, PIECES):
            if stage == STAGES[0]:
                gain = after(gain, near[2][0])[0]
            if stage == STAGES[-1]:
                gain = after(gain, *ready)[0]
            xs = []
            for r in stage:
                held = [after(x, own)[0] for x in near[r]] if r else near[r]
                xs += near[r]
                xs += [swap(x, "expert", 1, f"rows{c}pair{r}") for c, x in enumerate(held)]
            count = len(xs) // (2 * len(stage))
            own, *other = expert_stage(
                first_expert, xs, count, gain, *weights, all_experts, pieces
            )
            gain = after(gain, own)[0]
            came = [swap(o, "expert", 1, f"sums{stage[0]}pair") for o in other]
            wide = d // pieces
            for i, r in enumerate(stage):
                chip = [
                    own[i][:, n * wide : (n + 1) * wide].astype(F32) + came[n][i].astype(F32)
                    for n in range(pieces)
                ]
                if r in (1, 2):
                    chip = jnp.concatenate(chip, axis=1).astype(BF)
                    ready.append(chip)
                    chip = swap(chip, "expert", 2 * r, f"sums{r}chip")
                    landed.append(chip)
                    chip = [chip.astype(F32)]
                elif r == 3:
                    chip = [c.astype(BF) for c in chip]
                    half = pieces // 2
                    chip[half:] = after(*chip[half:], *landed)[:half]
                    chip = [swap(c, "expert", 2 * r, f"sums{r}chip").astype(F32) for c in chip]
                sums.append(jnp.concatenate(chip, axis=1))
        expert_out = sum(sums).astype(BF)
    else:
        order = jnp.arange(group, dtype=jnp.int32) ^ own_ep
        x = lax.all_gather(jnp.concatenate(mixed, axis=1), "expert", axis=0)[order]
        sums = []
        for p in range(0, group, 8):
            xs = [x[p + i] for i in range(8)]
            own, *other = expert_stage(first_expert, xs, 1, gain, *weights, all_experts, 1)
            other = jnp.concatenate(other, axis=2)
            sums.append(jnp.stack([own, other], axis=1).reshape(8, rows, d))
        part = jnp.concatenate(sums, axis=0)[order]
        expert_out = lax.psum_scatter(part, "expert", scatter_dimension=0)
    return (mixer_out, expert_out, next_state)


def solution(mesh):
    both = ("dp", "expert")
    rows = P(both, None)
    placed = (
        rows,
        rows,
        rows,
        rows,
        rows,
        P(None, both),
        P(None, both),
        P(),
        P(),
        P(both, None, None, None, None),
        P(both),
        P(both),
        rows,
        rows,
        P("expert", None, None),
        P("expert", None, None),
        P("expert", None, None),
    )
    return jax.shard_map(
        local,
        mesh=mesh,
        in_specs=placed,
        out_specs=(rows, rows, P(both, None, None, None)),
        check_vma=False,
    )
```

```python
import jax
import jax.numpy as jnp
from jax import lax
from jax.experimental import pallas as pl
from jax.experimental.pallas import tpu as pltpu
from jax.sharding import PartitionSpec as P

MOST = 56
PAIR = 2 * MOST
EPS = 1e-06
HEADS_A_STEP = 4
HEAD_CHUNKS = (8, 8)
STAGES = ((0,), (1, 2), (3,))
PIECES = (1, 2, 4)
LANES = 128
FAR = -100000.0
BF = jnp.bfloat16
F32 = jnp.float32
MIB = 1024 * 1024


def iota(shape, dim):
    return lax.broadcasted_iota(jnp.int32, shape, dim)


def mm(a, b):
    return jnp.dot(a, b, preferred_element_type=F32)


def silu(x):
    return x / (1.0 + jnp.exp(-x))


def prepare_kernel(*refs, carried):
    q_ref, k_ref, lb_ref, lbt_ref = refs[:4]
    from_refs, refs = refs[4 : 4 + carried], refs[4 + carried :]
    kq_ref, t_ref, mk_ref = refs[:3]
    to_refs, sems = refs[3 : 3 + carried], refs[3 + carried]
    copies = [pltpu.make_async_copy(a, b, sems.at[n]) for n, (a, b) in enumerate(zip(from_refs, to_refs))]

    @pl.when(pl.program_id(0) == 0)
    def _():
        for copy in copies:
            copy.start()

    rows = q_ref.shape[0]
    dk = 128
    at_row = iota((rows, rows), 0)
    at_col = iota((rows, rows), 1)
    strict = at_row > at_col
    inclusive = at_row >= at_col
    lower = inclusive.astype(F32)
    upper = (at_row <= at_col).astype(F32)
    top = lax.Precision.HIGHEST
    total_row = jnp.dot(lb_ref[0], upper, precision=top, preferred_element_type=F32)
    total_col = jnp.dot(lower, lbt_ref[0], precision=top, preferred_element_type=F32)
    solved = []
    mixes = []
    for i in range(HEADS_A_STEP):
        span = slice(i * dk, (i + 1) * dk)
        q = q_ref[:, span].astype(F32)
        k = k_ref[:, span].astype(F32)
        q = q / jnp.sqrt(jnp.sum(q * q, axis=-1, keepdims=True) + EPS)
        k = k / jnp.sqrt(jnp.sum(k * k, axis=-1, keepdims=True) + EPS)
        l_col = total_col[:, i : i + 1]
        l_row = total_row[i : i + 1, :]
        beta = lbt_ref[0][:, HEADS_A_STEP + i : HEADS_A_STEP + i + 1]
        ratio = jnp.where(inclusive, jnp.exp(jnp.where(inclusive, l_col - l_row, 0.0)), 0.0)
        kb = k.astype(BF)
        both = lax.dot_general(
            jnp.concatenate([kb, q.astype(BF)], axis=0),
            kb,
            (((1,), (1,)), ((), ())),
            preferred_element_type=F32,
        )
        mix = jnp.where(strict, beta * ratio * both[:rows], 0.0)
        growth = jnp.exp(l_col)
        trail = jnp.exp(l_col[rows - 1 : rows, :] - l_col)
        kq_ref[i] = jnp.concatenate([k * (beta * growth), q * growth], axis=0).astype(BF)
        mk_ref[i] = jnp.concatenate(
            [ratio * both[rows:], jnp.transpose(k * trail)], axis=0
        ).astype(BF)
        mixes.append(mix)
        first = (at_row // 2 == at_col // 2) & strict
        solved.append((at_row == at_col).astype(F32) - jnp.where(first, mix, 0.0))
    size = 2
    while size < rows:
        here = (
            (at_row // (2 * size) == at_col // (2 * size))
            & ((at_row // size) % 2 == 1)
            & ((at_col // size) % 2 == 0)
        )
        for i in range(HEADS_A_STEP):
            t = solved[i].astype(BF)
            block = jnp.where(here, mixes[i], 0.0).astype(BF)
            solved[i] = solved[i] - mm(t, mm(block, t).astype(BF))
        size *= 2
    for i in range(HEADS_A_STEP):
        t_ref[i] = solved[i].astype(BF)

    @pl.when(pl.program_id(0) == pl.num_programs(0) - 1)
    def _():
        for copy in copies:
            copy.wait()


def prepare(queries, keys_in, lb, lbt, first, heads, carry):
    rows = queries.shape[0]
    groups = heads // HEADS_A_STEP
    base = first // HEADS_A_STEP
    wide = HEADS_A_STEP * 128
    carry = [pltpu.with_memory_space_constraint(w, pltpu.HBM) for w in carry]
    kq, t, mk, *carried = pl.pallas_call(
        lambda *refs: prepare_kernel(*refs, carried=len(carry)),
        grid=(groups,),
        in_specs=[
            pl.BlockSpec((rows, wide), lambda i: (0, base + i)),
            pl.BlockSpec((rows, wide), lambda i: (0, base + i)),
            pl.BlockSpec((1,) + lb.shape[1:], lambda i: (base + i, 0, 0)),
            pl.BlockSpec((1,) + lbt.shape[1:], lambda i: (base + i, 0, 0)),
        ]
        + [pl.BlockSpec(memory_space=pl.ANY)] * len(carry),
        out_specs=[
            pl.BlockSpec((HEADS_A_STEP, 2 * rows, 128), lambda i: (i, 0, 0)),
            pl.BlockSpec((HEADS_A_STEP, rows, rows), lambda i: (i, 0, 0)),
            pl.BlockSpec((HEADS_A_STEP, rows + 128, rows), lambda i: (i, 0, 0)),
        ]
        + [pl.BlockSpec(memory_space=pltpu.VMEM)] * len(carry),
        out_shape=[
            jax.ShapeDtypeStruct((heads, 2 * rows, 128), BF),
            jax.ShapeDtypeStruct((heads, rows, rows), BF),
            jax.ShapeDtypeStruct((heads, rows + 128, rows), BF),
        ]
        + [pltpu.VMEM(w.shape, w.dtype) for w in carry],
        scratch_shapes=[pltpu.SemaphoreType.DMA((max(1, len(carry)),))],
        compiler_params=pltpu.CompilerParams(vmem_limit_bytes=12 * MIB),
        cost_estimate=pl.CostEstimate(flops=1000, transcendentals=0, bytes_accessed=1000),
        name="prepare",
    )(queries, keys_in, lb, lbt, *carry)
    return kq, t, mk, carried


def pack_kernel(own_ref, *refs, peers, first):
    asked, cache_ref, outs = refs[:peers], refs[peers], refs[peers + 1 : 2 * peers + 1]
    buf, sems = refs[2 * peers + 1 :]
    heads = buf.shape[1]
    copies = []
    for j in range(peers):
        slot = jnp.where(asked[j][0] == own_ref[0], asked[j][1], 0)
        copies.append(
            pltpu.make_async_copy(
                cache_ref.at[0, slot, pl.ds(first, heads)], buf.at[j], sems.at[j]
            )
        )
        copies[-1].start()
    for j in range(peers):
        copies[j].wait()
        outs[j][...] = buf[j].astype(BF)


def pack(own, asked, cache, first, heads):
    peers = len(asked)
    shape = (heads,) + cache.shape[3:]
    return pl.pallas_call(
        lambda *refs: pack_kernel(*refs, peers=peers, first=first),
        grid_spec=pltpu.PrefetchScalarGridSpec(
            num_scalar_prefetch=1 + peers,
            grid=(1,),
            in_specs=[pl.BlockSpec(memory_space=pl.ANY)],
            out_specs=[pl.BlockSpec(shape, lambda i, *p: (0, 0, 0))] * peers,
            scratch_shapes=[
                pltpu.VMEM((peers,) + shape, F32),
                pltpu.SemaphoreType.DMA((peers,)),
            ],
        ),
        out_shape=[jax.ShapeDtypeStruct(shape, BF)] * peers,
        compiler_params=pltpu.CompilerParams(vmem_limit_bytes=12 * MIB),
        cost_estimate=pl.CostEstimate(flops=1000, transcendentals=0, bytes_accessed=1000),
        name="pack",
    )(own, *asked, cache)


def resume_kernel(pick_ref, *refs, peers, first_head, experts, carried):
    cache_ref, got_refs, refs = refs[0], refs[1 : 1 + peers], refs[1 + peers :]
    kq_ref, t_ref, mk_ref, v_ref, lb_ref, lbt_ref, gate_ref, res_ref, gain_ref = refs[:9]
    ids_ref, weight_ref = refs[9:11]
    from_refs, refs = refs[11 : 11 + carried], refs[11 + carried :]
    out_ref, next_ref = refs[:2]
    to_refs, refs = refs[2 : 2 + carried], refs[2 + carried :]
    own_buf, got_buf, sem_own, sem_got, sem_carry = refs
    copies = [
        pltpu.make_async_copy(a, b, sem_carry.at[n])
        for n, (a, b) in enumerate(zip(from_refs, to_refs))
    ]
    heads, rows, _ = t_ref.shape
    steps = own_buf.shape[0] // heads
    at = pl.program_id(0)
    place = pick_ref[0]
    slot = pick_ref[1]

    def own_copy(s):
        return pltpu.make_async_copy(
            cache_ref.at[0, slot, pl.ds(first_head + s * heads, heads)],
            own_buf.at[pl.ds(s * heads, heads)],
            sem_own.at[s],
        )

    def got_copy(s, j):
        return pltpu.make_async_copy(
            got_refs[j].at[pl.ds(s * heads, heads)],
            got_buf.at[pl.ds(s * heads, heads)],
            sem_got.at[s],
        )

    @pl.when(at == 0)
    def _():
        for s in range(steps):
            own_copy(s).start()
            for j in range(peers):

                @pl.when(place == j + 1)
                def _(s=s, j=j):
                    got_copy(s, j).start()

        for copy in copies:
            copy.start()
        if experts:
            line = iota((LANES, rows), 0)
            named = jnp.zeros((LANES, rows), F32)
            for k in range(ids_ref.shape[0]):
                hit = line % experts == ids_ref[k : k + 1, :]
                named = jnp.where(hit, weight_ref[k : k + 1, :], named)
            coarse = named.astype(BF).astype(F32)
            both = jnp.where(line < experts, coarse, named - coarse)
            both = jnp.where(line < 2 * experts, both, 0.0)
            out_ref[:, out_ref.shape[1] - LANES :] = jnp.transpose(both).astype(BF)

    own_copy(at).wait()

    @pl.when(place > 0)
    def _():
        got_copy(at, 0).wait()

    here = place == 0
    for i in range(heads):
        span = slice(i * 128, (i + 1) * 128)
        head = at * heads + i
        state = jnp.where(here, own_buf[head], got_buf[head].astype(F32))
        beta = lbt_ref[0][:, HEADS_A_STEP + i : HEADS_A_STEP + i + 1]
        read = mm(kq_ref[i], state.astype(BF))
        rest = beta * v_ref[:, span].astype(F32) - read[:rows]
        fixed = mm(t_ref[i], rest.astype(BF)).astype(BF)
        added = mm(mk_ref[i], fixed)
        o = read[rows:] + added[:rows]
        last = jnp.exp(jnp.sum(lb_ref[0][i : i + 1, :], axis=-1, keepdims=True))
        next_ref[i] = last * state + added[rows:]
        scaled = o / jnp.sqrt(jnp.mean(o * o, axis=-1, keepdims=True) + EPS) * gain_ref[...]
        gated = scaled * silu(gate_ref[:, span].astype(F32))
        mixed = (res_ref[:, span].astype(F32) + gated).astype(BF)
        out_ref[:, pl.ds(pl.multiple_of(head * 128, 128), 128)] = mixed

    @pl.when(at == steps - 1)
    def _():
        for copy in copies:
            copy.wait()


def resume(
    pick, cache, got, kq, t, mk, values, lb, lbt, gate, residual, gain, ids, weight, first, heads,
    experts, carry,
):
    rows = values.shape[0]
    step = HEADS_A_STEP
    carry = [pltpu.with_memory_space_constraint(w, pltpu.HBM) for w in carry]
    wide = heads * 128 + (LANES if experts else 0)
    base = first // step
    any_spec = pl.BlockSpec(memory_space=pl.ANY)
    cols = pl.BlockSpec((rows, step * 128), lambda i, p: (0, base + i))
    group = lambda i, p: (base + i, 0, 0)
    local_group = lambda i, p: (i, 0, 0)
    whole = lambda i, p: (0, 0)
    out, state, *carried = pl.pallas_call(
        lambda *refs: resume_kernel(
            *refs, peers=len(got), first_head=first, experts=experts, carried=len(carry)
        ),
        grid_spec=pltpu.PrefetchScalarGridSpec(
            num_scalar_prefetch=1,
            grid=(heads // step,),
            in_specs=[any_spec]
            + [any_spec] * len(got)
            + [
                pl.BlockSpec((step,) + kq.shape[1:], local_group),
                pl.BlockSpec((step,) + t.shape[1:], local_group),
                pl.BlockSpec((step,) + mk.shape[1:], local_group),
                cols,
                pl.BlockSpec((1,) + lb.shape[1:], group),
                pl.BlockSpec((1,) + lbt.shape[1:], group),
                cols,
                cols,
                pl.BlockSpec((1, 128), whole),
                pl.BlockSpec(ids.shape, whole),
                pl.BlockSpec(weight.shape, whole),
            ]
            + [any_spec] * len(carry),
            out_specs=[
                pl.BlockSpec((rows, wide), whole),
                pl.BlockSpec((step, 128, 128), lambda i, p: (i, 0, 0)),
            ]
            + [pl.BlockSpec(memory_space=pltpu.VMEM)] * len(carry),
            scratch_shapes=[
                pltpu.VMEM((heads, 128, 128), F32),
                pltpu.VMEM((heads, 128, 128), BF),
                pltpu.SemaphoreType.DMA((heads // step,)),
                pltpu.SemaphoreType.DMA((heads // step,)),
                pltpu.SemaphoreType.DMA((max(1, len(carry)),)),
            ],
        ),
        out_shape=[
            jax.ShapeDtypeStruct((rows, wide), BF),
            jax.ShapeDtypeStruct((heads, 128, 128), F32),
        ]
        + [pltpu.VMEM(w.shape, w.dtype) for w in carry],
        compiler_params=pltpu.CompilerParams(vmem_limit_bytes=12 * MIB),
        cost_estimate=pl.CostEstimate(flops=1000, transcendentals=0, bytes_accessed=1000),
        name="resume",
    )(pick, cache, *got, kq, t, mk, values, lb, lbt, gate, residual, gain, ids, weight, *carry)
    return out, state, carried


def expert_kernel(first_ref, *refs, blocks, parts, experts, all_experts, pieces):
    x_refs, refs = refs[: blocks * parts], refs[blocks * parts :]
    gain_ref, wg_ref, wu_ref, wd_ref, own_ref = refs[:5]
    other_refs, refs = refs[5 : 5 + pieces], refs[5 + pieces :]
    xs_ref, posr_ref, posc_ref, wr_ref, chosen_ref, slot_ref, rows_ref = refs
    step = pl.program_id(0)
    e = step
    rows = x_refs[0].shape[0]
    d = xs_ref.shape[1]
    pairs = blocks // 2
    two = 2 * rows

    @pl.when(step == 0)
    def _():
        gain = gain_ref[...]
        slab = 16
        a, b = iota((LANES, LANES), 0), iota((LANES, LANES), 1)
        first = first_ref[0]
        mine = ((a == first + b) | (a == first + b + all_experts)) & (b < experts)
        mine = mine.astype(F32).astype(BF)
        before = (iota((rows, rows), 0) > iota((rows, rows), 1)).astype(F32).astype(BF)
        for n in range(blocks):
            last = x_refs[n * parts + parts - 1]
            weight = mm(last[:, last.shape[1] - LANES :], mine)
            routed = weight > 0.0
            rank = mm(before, routed.astype(F32).astype(BF)) + float(n % 2 * MOST)
            rank = jnp.where(routed, rank, FAR)
            posc_ref[n] = rank
            posr_ref[n] = jnp.transpose(rank)
            wr_ref[n] = jnp.transpose(weight)

            def norm(s, carry, n=n):
                at = pl.multiple_of(s * slab, slab)
                pieces = [x_refs[n * parts + c][pl.ds(at, slab), :] for c in range(parts)]
                pieces[-1] = pieces[-1][:, : pieces[-1].shape[1] - LANES]
                x = jnp.concatenate(pieces, axis=1).astype(F32)
                mean = jnp.mean(x * x, axis=-1, keepdims=True)
                to = pl.multiple_of(n * rows + s * slab, slab)
                xs_ref[pl.ds(to, slab), :] = (x * (1.0 / jnp.sqrt(mean + EPS)) * gain).astype(BF)
                return carry

            lax.fori_loop(0, rows // slab, norm, 0, unroll=8)

    if True:
        for p in range(pairs):
            pos = [posr_ref[2 * p + c, pl.ds(e, 1), :] for c in range(2)]
            weight = [wr_ref[2 * p + c, pl.ds(e, 1), :] for c in range(2)]
            sel = iota((PAIR, two), 0).astype(F32) == jnp.concatenate(pos, axis=1)
            span = slice(p * PAIR, (p + 1) * PAIR)
            slot_ref[span, :] = jnp.broadcast_to(
                jnp.sum(
                    jnp.where(sel, jnp.concatenate(weight, axis=1), 0.0), axis=1, keepdims=True
                ),
                (PAIR, LANES),
            )
            chosen_ref[span, :] = mm(
                sel.astype(F32).astype(BF), xs_ref[p * two : (p + 1) * two, :]
            ).astype(BF)

    x = chosen_ref[...]
    hidden = silu(mm(x, wg_ref[e])) * mm(x, wu_ref[e]) * slot_ref[:, 0:1]
    done = mm(hidden.astype(BF), wd_ref[e]).astype(BF)
    to = pl.multiple_of(e * PAIR, 16)
    for p in range(pairs):
        rows_ref[p, pl.ds(to, PAIR), :] = done[p * PAIR : (p + 1) * PAIR]

    @pl.when(step == pl.num_programs(0) - 1)
    def _():
        lane = iota((two, experts * PAIR), 1).astype(F32)
        for p in range(pairs):
            at = jnp.concatenate([posc_ref[2 * p], posc_ref[2 * p + 1]], axis=0)
            hit = lane == at[:, 0:1]
            for n in range(1, experts):
                hit = hit | (lane == at[:, n : n + 1] + float(n * PAIR))
            both = mm(hit.astype(F32).astype(BF), rows_ref[p]).astype(BF)
            own_ref[p] = both[:rows]
            for n in range(pieces):
                other_refs[n][p] = both[rows:, n * d // pieces : (n + 1) * d // pieces]


def expert_stage(first, xs, parts, gain, w_gate, w_up, w_down, all_experts, pieces):
    experts, d, ff = w_gate.shape
    rows = xs[0].shape[0]
    blocks = len(xs) // parts
    pairs = blocks // 2
    one = pl.Buffered(1)
    outs = [jax.ShapeDtypeStruct((pairs, rows, d), BF)]
    outs += [jax.ShapeDtypeStruct((pairs, rows, d // pieces), BF)] * pieces
    whole3 = lambda s, m: (0, 0, 0)
    return pl.pallas_call(
        lambda *refs: expert_kernel(
            *refs, blocks=blocks, parts=parts, experts=experts, all_experts=all_experts,
            pieces=pieces,
        ),
        grid_spec=pltpu.PrefetchScalarGridSpec(
            num_scalar_prefetch=1,
            grid=(experts,),
            in_specs=[pl.BlockSpec(x.shape, lambda s, m: (0, 0), pipeline_mode=one) for x in xs]
            + [
                pl.BlockSpec((1, d), lambda s, m: (0, 0)),
                pl.BlockSpec(memory_space=pltpu.VMEM),
                pl.BlockSpec(memory_space=pltpu.VMEM),
                pl.BlockSpec(memory_space=pltpu.VMEM),
            ],
            out_specs=[pl.BlockSpec(out.shape, whole3) for out in outs],
            scratch_shapes=[
                pltpu.VMEM((blocks * rows, d), BF),
                pltpu.VMEM((blocks, LANES, rows), F32),
                pltpu.VMEM((blocks, rows, LANES), F32),
                pltpu.VMEM((blocks, LANES, rows), F32),
                pltpu.VMEM((pairs * PAIR, d), BF),
                pltpu.VMEM((pairs * PAIR, LANES), F32),
                pltpu.VMEM((pairs, experts * PAIR, d), BF),
            ],
        ),
        out_shape=outs,
        compiler_params=pltpu.CompilerParams(vmem_limit_bytes=(4 + 5 * pairs) * MIB),
        cost_estimate=pl.CostEstimate(flops=1000, transcendentals=0, bytes_accessed=1000),
        name="experts",
    )(first, *xs, gain, w_gate, w_up, w_down)


def after(*xs):
    return lax.optimization_barrier(xs)


def swap(x, axis, bits, what):
    size = lax.axis_size(axis)
    with jax.named_scope(what):
        return lax.ppermute(x, axis, [(i, i ^ bits) for i in range(size)])


def local(
    residual_in,
    queries,
    keys_in,
    values_in,
    out_gate,
    log_decay,
    beta_rate,
    head_gain,
    moe_gain,
    state_cache,
    hit_holder,
    hit_slot,
    expert_ids,
    gate_weight,
    w_gate,
    w_up,
    w_down,
):
    rows, d = queries.shape
    head_count = log_decay.shape[0]
    queries, keys_in, values_in, out_gate, residual_in, state_cache, ids_t, weight_t, head_gain = (
        pltpu.with_memory_space_constraint(x, pltpu.HBM)
        for x in (
            queries, keys_in, values_in, out_gate, residual_in, state_cache, expert_ids.T,
            gate_weight.T, head_gain[None],
        )
    )
    holders = lax.axis_size("dp")
    group = lax.axis_size("expert")
    own_dp = lax.axis_index("dp")
    own_ep = lax.axis_index("expert")
    experts = w_gate.shape[0]
    pairs = group // 2
    all_experts = group * experts
    chunks = HEAD_CHUNKS
    starts = [sum(chunks[:g]) for g in range(len(chunks))]

    groups = head_count // HEADS_A_STEP
    lb = jnp.concatenate(
        [
            log_decay.reshape(groups, HEADS_A_STEP, rows),
            beta_rate.reshape(groups, HEADS_A_STEP, rows),
        ],
        axis=1,
    )
    lbt = lb.transpose(0, 2, 1)
    pick = jnp.stack([hit_holder[0] ^ own_dp, hit_slot[0]])

    wish = jnp.concatenate([hit_holder, hit_slot])
    asked = [swap(wish, "dp", j, f"hits{j}") for j in range(1, holders)]
    asked[0], lb, lbt, pick = after(asked[0], lb, lbt, pick)
    got = []
    for first, heads in zip(starts, chunks):
        pieces = pack(own_dp[None], asked, state_cache, first, heads)
        asked[0], *pieces = after(asked[0], *pieces)
        got.append(
            [swap(p, "dp", j + 1, f"state{first}from{j + 1}") for j, p in enumerate(pieces)]
        )

    lb = after(lb, asked[0])[0]
    mixed, states, held = [], [], []
    carry = {("prepare", 1): (w_up, w_down), ("resume", 1): (w_gate,)}
    for g, (first, heads) in enumerate(zip(starts, chunks)):
        last = g == len(chunks) - 1
        *ready, new = prepare(queries, keys_in, lb, lbt, first, heads, carry.pop(("prepare", g), ()))
        held += new
        kq, t, mk = ready
        more = carry.pop(("resume", g), ())
        m, s, new = resume(
            pick, state_cache, got[g], kq, t, mk, values_in, lb, lbt, out_gate, residual_in,
            head_gain, ids_t, weight_t, first, heads, all_experts if last else 0,
            more,
        )
        held += new
        pick, lb = after(pick, lb, m)[:2]
        mixed.append(m)
        states.append(s)
    parts = len(chunks)
    next_state = jnp.concatenate(states, axis=0)[None]
    mixer_out = jnp.concatenate(mixed[:-1] + [mixed[-1][:, :-LANES]], axis=1)

    gain = moe_gain[None]
    first_expert = (own_ep * experts)[None].astype(jnp.int32)
    weights = [held[n] for n in (2, 0, 1)]
    if group == 8:
        near = [mixed, [], [], []]
        for c in range(parts):
            near[2].append(swap(mixed[c], "expert", 4, f"rows{c}chip2"))
            near[3].append(swap(near[2][c], "expert", 2, f"rows{c}chip3"))
        for c in range(parts):
            x = after(mixed[c], mixed[-1])[0]
            near[1].append(swap(x, "expert", 2, f"rows{c}chip1"))
        sums, ready, landed = [], [], []
        gain, mixer_out, next_state = after(gain, mixer_out, next_state)
        for stage, pieces in zip(STAGES, PIECES):
            if stage == STAGES[0]:
                gain = after(gain, near[2][0])[0]
            if stage == STAGES[-1]:
                gain = after(gain, *ready)[0]
            xs = []
            for r in stage:
                held = [after(x, own)[0] for x in near[r]] if r else near[r]
                xs += near[r]
                xs += [swap(x, "expert", 1, f"rows{c}pair{r}") for c, x in enumerate(held)]
            count = len(xs) // (2 * len(stage))
            own, *other = expert_stage(
                first_expert, xs, count, gain, *weights, all_experts, pieces
            )
            gain = after(gain, own)[0]
            came = [swap(o, "expert", 1, f"sums{stage[0]}pair") for o in other]
            wide = d // pieces
            for i, r in enumerate(stage):
                chip = [
                    own[i][:, n * wide : (n + 1) * wide].astype(F32) + came[n][i].astype(F32)
                    for n in range(pieces)
                ]
                if r in (1, 2):
                    chip = jnp.concatenate(chip, axis=1).astype(BF)
                    ready.append(chip)
                    chip = swap(chip, "expert", 2 * r, f"sums{r}chip")
                    if r == 2:
                        landed.append(chip)
                    chip = [chip.astype(F32)]
                elif r == 3:
                    chip = [c.astype(BF) for c in chip]
                    half = pieces // 2
                    chip[half:] = after(*chip[half:], *landed)[:half]
                    chip = [swap(c, "expert", 2 * r, f"sums{r}chip").astype(F32) for c in chip]
                sums.append(jnp.concatenate(chip, axis=1))
        expert_out = sum(sums).astype(BF)
    else:
        order = jnp.arange(group, dtype=jnp.int32) ^ own_ep
        x = lax.all_gather(jnp.concatenate(mixed, axis=1), "expert", axis=0)[order]
        sums = []
        for p in range(0, group, 8):
            xs = [x[p + i] for i in range(8)]
            own, *other = expert_stage(first_expert, xs, 1, gain, *weights, all_experts, 1)
            other = jnp.concatenate(other, axis=2)
            sums.append(jnp.stack([own, other], axis=1).reshape(8, rows, d))
        part = jnp.concatenate(sums, axis=0)[order]
        expert_out = lax.psum_scatter(part, "expert", scatter_dimension=0)
    return (mixer_out, expert_out, next_state)


def solution(mesh):
    both = ("dp", "expert")
    rows = P(both, None)
    placed = (
        rows,
        rows,
        rows,
        rows,
        rows,
        P(None, both),
        P(None, both),
        P(),
        P(),
        P(both, None, None, None, None),
        P(both),
        P(both),
        rows,
        rows,
        P("expert", None, None),
        P("expert", None, None),
        P("expert", None, None),
    )
    return jax.shard_map(
        local,
        mesh=mesh,
        in_specs=placed,
        out_specs=(rows, rows, P(both, None, None, None)),
        check_vma=False,
    )
```
